256 devices in a mesh: expert: 8 (over x, core), dp: 32 (over y, z).
Axes of the slice: x: 4, y: 4, z: 8, core: 2. Of those that a mesh axis runs over, the one named last changes fastest.
Arguments:
- tokens: bfloat16 [32768, 1024], P(('expert', 'dp')), may hold values from -6 to 6
- norm_gain: float32 [1024], replicated, may hold values from 0.1 to 1.9
- router_weight: bfloat16 [1024, 8], replicated, may hold values from -0.3984375 to 0.3984375
- shared_gate_vector: float32 [1024], replicated, may hold values from -0.4 to 0.4
- expert_ids: int32 [32768, 2], P(('expert', 'dp')), may hold values from 0 to 7, all different within a row; in each aligned block of 128 rows (0 to 127, 128 to 255, ...) at most 48 rows name the same one
- gate_weight: bfloat16 [8, 1024, 4096], P('expert', None, 'dp'), may hold values from -0.1875 to 0.1875
- up_weight: bfloat16 [8, 1024, 4096], P('expert', None, 'dp'), may hold values from -0.1875 to 0.1875
- down_weight: bfloat16 [8, 1024, 4096], P('expert', None, 'dp'), may hold values from -0.09375 to 0.09375
- shared_gate_weight: bfloat16 [1024, 4096], P(None, 'expert'), may hold values from -0.1875 to 0.1875
- shared_up_weight: bfloat16 [1024, 4096], P(None, 'expert'), may hold values from -0.1875 to 0.1875
- shared_down_weight: bfloat16 [4096, 1024], P('expert'), may hold values from -0.09375 to 0.09375
Outputs:
- mixed: bfloat16 [32768, 1024], P(('expert', 'dp'))
The draws below stay inside these ranges and needn't reach their ends.
Inputs may be any that keep to these rules, and one draw needn't show every extreme that they name: `expert_ids`: in each aligned block of 128 rows (the rows of one device) no expert is named by more than 48 pairs, and in some block one expert is named by exactly 48; the two ids of a row differ.
All inputs are finite; a program needn't handle non-finite values.
Results may differ from the reference program's by a relative error of at most 0.0085.
Values may be sent and summed in bfloat16 or wider, within the bound.
A program may use at most 128 MiB of HBM per device.

```python
import math
import jax
import jax.numpy as jnp
import numpy as np
from jax import lax

D = 1024
FF = 4096
SFF = 4096
TOK_DEV = 128
EXPERTS = 8
CAP = 48
TOKENS = 32768
N_EXPERT = 8


def shard_levels(stream_key, extent, shards, least, top_value):
    factor_of = 1.0
    for axis_at, parts in shards:
        steps = jax.random.uniform(jax.random.fold_in(jax.random.fold_in(stream_key, 6), axis_at), (parts,), jnp.float32, least / len(shards), top_value / len(shards))
        factor_of = factor_of * jnp.repeat(jnp.exp(steps), extent[axis_at] // parts).reshape((-1,) + (1,) * (len(extent) - 1 - axis_at))
    return factor_of


def routed_block(rng, own, number, rows, count, top, reach, skew):
    sequence = jax.random.permutation(rng, count)
    heavy_load, common = shares(count, rows * top, reach, skew, True), shares(count, rows * top, reach, skew, False)
    places = jnp.arange(count)

    def named(tallies, rotation):
        used = int((tallies > 0).sum())
        fixed = max(1, used // 4)
        shifted = fixed + (places - fixed + rotation * (used - fixed)) % max(1, count - fixed)
        return jnp.zeros((count,), jnp.int32).at[sequence[jnp.where(places < fixed, places, shifted)]].set(jnp.asarray(tallies, jnp.int32))

    tallies = jnp.where(number % 4 == 0, named(heavy_load, number // 4), named(common, number - number // 4 - 1))
    mixed = jax.random.permutation(jax.random.fold_in(own, 3), count)
    donor, receiver = mixed[0:count // 2 * 2:2], mixed[1:count // 2 * 2:2]
    room = jnp.minimum(tallies[donor] - 1, reach - tallies[receiver]) // 2
    room = jnp.where((donor == sequence[0]) | (receiver == sequence[0]) | (tallies[receiver] == 0), 0, jnp.maximum(room, 0))
    shifted = jax.random.randint(jax.random.fold_in(own, 4), (count // 2,), 0, 1 << 20) % (room + 1)
    tallies = tallies.at[donor].add(-shifted).at[receiver].add(shifted)
    items = jnp.searchsorted(jnp.cumsum(tallies), jnp.arange(rows * top), side="right").astype(jnp.int32)
    listing = items.reshape(top, rows).T
    listing = listing[jax.random.permutation(jax.random.fold_in(own, 1), rows)]
    rotation = jax.random.randint(jax.random.fold_in(own, 2), (rows, 1), 0, top)
    return jnp.take_along_axis(listing, (jnp.arange(top)[None, :] + rotation) % top, axis=1)


def shares(number_of, total, bound, lean, full):
    portions = [(1 << 20) // math.isqrt(rank ** lean) + 1 for rank in range(1, number_of + 1)]
    largest = bound if full else min(bound, max(-(-total // number_of), total * portions[0] // sum(portions)))
    least = 1 if total - largest >= number_of - 1 else 0
    holding, surplus = [largest] + [least] * (number_of - 1), total - largest - least * (number_of - 1)
    while surplus > 0:
        movable = [i for i in range(1, number_of) if holding[i] < largest] or [i for i in range(1, number_of) if holding[i] < bound]
        mass, remaining = sum([portions[i] for i in movable]), surplus
        for i in movable:
            addition = min(bound - holding[i], max(1, remaining * portions[i] // mass), surplus)
            holding[i] = holding[i] + addition
            surplus = surplus - addition
    return np.array(holding)


def bell_draw(own_key, shape, spread, limit, cuts=(), kind=jnp.bfloat16):
    values = spread * jax.random.normal(own_key, shape, jnp.float32)
    if cuts:
        values = values * shard_levels(own_key, shape, cuts, -0.22, 0.18)
    return jnp.clip(values, -limit, limit).astype(kind)


def setup_inputs(seed: int = 0) -> dict:
    arg_keys = jax.random.split(jax.random.key(seed), 12)
    tokens = bell_draw(arg_keys[0], (TOKENS, D), 1.0, 6.0, ((0, 256),))
    norm_gain = jnp.clip(1.0 + 0.18 * jax.random.normal(arg_keys[1], (D,), jnp.float32), 0.1, 1.9)
    router_weight = bell_draw(arg_keys[2], (D, EXPERTS), 0.0625, 0.3984375)
    shared_gate_vector = bell_draw(arg_keys[3], (D,), 0.0625, 0.4, (), jnp.float32)
    expert_ids_keys = jax.random.split(jax.random.fold_in(arg_keys[4], 1), TOKENS // TOK_DEV)
    expert_ids_turns = jax.random.permutation(jax.random.fold_in(arg_keys[4], 3), TOKENS // TOK_DEV)
    expert_ids = jax.vmap(lambda own, number: routed_block(jax.random.fold_in(arg_keys[4], 2), own, number, TOK_DEV, EXPERTS, 2, CAP, 2))(expert_ids_keys, expert_ids_turns).reshape((TOKENS, 2))
    gate_weight = bell_draw(arg_keys[5], (EXPERTS, D, FF), D ** -0.5, 0.1875, ((0, 8), (2, 32)))
    up_weight = bell_draw(arg_keys[6], (EXPERTS, D, FF), D ** -0.5, 0.1875, ((0, 8), (2, 32)))
    down_weight = bell_draw(arg_keys[7], (EXPERTS, D, FF), FF ** -0.5, 0.09375, ((0, 8), (2, 32)))
    shared_gate_weight = bell_draw(arg_keys[8], (D, SFF), D ** -0.5, 0.1875, ((1, 8),))
    shared_up_weight = bell_draw(arg_keys[9], (D, SFF), D ** -0.5, 0.1875, ((1, 8),))
    shared_down_weight = bell_draw(arg_keys[10], (SFF, D), SFF ** -0.5, 0.09375, ((0, 8),))
    return dict(tokens=tokens, norm_gain=norm_gain, router_weight=router_weight, shared_gate_vector=shared_gate_vector, expert_ids=expert_ids, gate_weight=gate_weight, up_weight=up_weight, down_weight=down_weight, shared_gate_weight=shared_gate_weight, shared_up_weight=shared_up_weight, shared_down_weight=shared_down_weight)


def rms_norm(values, gain):
    floats = values.astype(jnp.float32)
    mean_square = lax.optimization_barrier(jnp.mean(floats * floats, axis=-1, keepdims=True))
    return (floats * lax.rsqrt(mean_square + 1e-06) * gain).astype(jnp.bfloat16)

def routing(normed, router_weight, expert_ids):
    logits = jnp.dot(normed, router_weight, preferred_element_type=jnp.float32)
    onehot = expert_ids[:, :, None] == jnp.arange(router_weight.shape[1], dtype=jnp.int32)[None, None, :]
    picked = lax.optimization_barrier(jnp.sum(jnp.where(onehot, logits[:, None, :], jnp.float32(0.0)), axis=-1))
    first_weight = jax.nn.sigmoid(picked[:, 0] - picked[:, 1])
    return jnp.stack([first_weight, 1.0 - first_weight], axis=1)

def slot_of(block_ids):
    flat_ids = block_ids.reshape(-1)
    onehot = (flat_ids[:, None] == jnp.arange(EXPERTS, dtype=jnp.int32)[None, :]).astype(jnp.int32)
    before = jnp.cumsum(onehot, axis=0) - onehot
    return lax.optimization_barrier(jnp.sum(before * onehot, axis=1)).reshape(block_ids.shape).astype(jnp.int32)

def reference(tokens, norm_gain, router_weight, shared_gate_vector, expert_ids, gate_weight, up_weight, down_weight, shared_gate_weight, shared_up_weight, shared_down_weight):
    normed = rms_norm(tokens, norm_gain)
    route_weight = routing(normed, router_weight, expert_ids)
    num_blocks = TOKENS // TOK_DEV
    slot = jax.vmap(slot_of)(expert_ids.reshape(num_blocks, TOK_DEV, 2)).reshape(TOKENS, 2)
    source_block = (jnp.arange(TOKENS, dtype=jnp.int32) // TOK_DEV).astype(jnp.int32)
    position = (source_block[:, None] * CAP + slot).astype(jnp.int32)
    padded_rows = num_blocks * CAP

    def expert_step(running, expert_index):
        slot_index = jnp.where(expert_ids == expert_index, position, padded_rows).astype(jnp.int32)
        buffer = jnp.zeros((padded_rows, D), jnp.bfloat16)
        buffer = buffer.at[slot_index[:, 0]].set(normed, mode='drop')
        buffer = buffer.at[slot_index[:, 1]].set(normed, mode='drop')
        gate_part = jnp.dot(buffer, gate_weight[expert_index], preferred_element_type=jnp.float32)
        up_part = jnp.dot(buffer, up_weight[expert_index], preferred_element_type=jnp.float32)
        hidden = (jax.nn.silu(gate_part) * up_part).astype(jnp.bfloat16)
        expert_out = lax.dot_general(hidden, down_weight[expert_index], (((1,), (1,)), ((), ())), preferred_element_type=jnp.float32).astype(jnp.bfloat16)
        for column in range(2):
            fetched = expert_out[jnp.minimum(slot_index[:, column], padded_rows - 1)].astype(jnp.float32)
            scale = jnp.where(expert_ids[:, column] == expert_index, route_weight[:, column], jnp.float32(0.0))
            running = running + scale[:, None] * fetched
        return (running, None)
    routed, _ = lax.scan(expert_step, jnp.zeros((TOKENS, D), jnp.float32), jnp.arange(EXPERTS, dtype=jnp.int32))
    block_units = SFF // N_EXPERT
    shared = jnp.zeros((TOKENS, D), jnp.float32)
    for block_index in range(N_EXPERT):
        lower = block_index * block_units
        gate_part = jnp.dot(normed, shared_gate_weight[:, lower:lower + block_units], preferred_element_type=jnp.float32)
        up_part = jnp.dot(normed, shared_up_weight[:, lower:lower + block_units], preferred_element_type=jnp.float32)
        hidden = (jax.nn.silu(gate_part) * up_part).astype(jnp.bfloat16)
        partial_out = jnp.dot(hidden, shared_down_weight[lower:lower + block_units, :], preferred_element_type=jnp.float32).astype(jnp.bfloat16)
        partial_out = lax.optimization_barrier(partial_out)
        shared = shared + partial_out.astype(jnp.float32)
    shared_gate = jax.nn.sigmoid(lax.optimization_barrier(jnp.sum(normed.astype(jnp.float32) * shared_gate_vector, axis=-1)))
    return (routed + shared_gate[:, None] * shared).astype(jnp.bfloat16)
```

```python
import jax
import jax.numpy as jnp
from jax import lax
from jax.experimental import pallas as pl
from jax.experimental.pallas import tpu as pltpu
from jax.sharding import PartitionSpec as P

MESH = pl.DeviceIdType.MESH
BF16 = jnp.bfloat16
F32 = jnp.float32

XN, CN, YN, ZN = 4, 2, 4, 8
TOK = 128
D = 1024
HID = 128
SHID = 512
CAP = 48
BLOCKS = XN * CN
ROWS = BLOCKS * CAP
NC = 4
CW = D // NC
HALF_R = ROWS // 2
HALF_T = TOK // 2
COPIES = 256

NT = (((1,), (1,)), ((), ()))


def dot(a, b):
    return jnp.dot(a, b, preferred_element_type=F32)


class Links:
    def __init__(self, send_sem, recv_sem):
        self.send_sem, self.recv_sem = send_sem, recv_sem
        self.copies, self.started, self.arrived = {}, [], set()

    def add(self, name, src, dst, device):
        k = len(self.copies)
        self.copies[name] = pltpu.make_async_remote_copy(
            src_ref=src,
            dst_ref=dst,
            send_sem=self.send_sem.at[k],
            recv_sem=self.recv_sem.at[k],
            device_id=device,
            device_id_type=MESH,
        )

    def send(self, *name):
        self.copies[name].start()
        self.started.append(name)

    def arrive(self, *name):
        if name not in self.arrived:
            self.arrived.add(name)
            self.copies[name].wait_recv()

    def finish(self):
        assert set(self.started) == set(self.copies) == self.arrived
        for name in self.started:
            self.copies[name].wait_send()


def silu_mul(g, u):
    return (g * jax.nn.sigmoid(g) * u).astype(BF16)


def layer_kernel(
    tokens, ids, gain, router, gate_vector, gate, up, down, sgate, sup, sdown, out,
    tok, idt, xn, sel, wcol, gcol, rows, gu, dn, hid, sgw, suw, sdw, shared,
    yown, ymerge, ys1, ys2, ys3, yr1, yr2, yr3,
    cown, csend, crecv, xmerge, xs1, xs2, xs3, xr1, xr2, xr3,
    local_sem, send_sem, recv_sem,
):
    e, d = lax.axis_index("expert"), lax.axis_index("dp")
    x, core = lax.div(e, CN), lax.rem(e, CN)
    y, z = lax.div(d, ZN), lax.rem(d, ZN)

    def step_x(by):
        return (lax.rem(x + by, XN) * CN + core, d)

    def step_y(by):
        return (e, lax.rem(y + by, YN) * ZN + z)

    def step_z(by):
        return (e, y * ZN + lax.rem(z + by, ZN))

    to_x = (step_x(1), step_x(XN - 1))
    to_y = (step_y(1), step_y(YN - 1))
    to_z = (step_z(1), step_z(ZN - 1))
    partner = (x * CN + (1 - core), d)

    local = [
        pltpu.make_async_copy(src, dst, local_sem.at[i])
        for i, (src, dst) in enumerate(
            (
                (tokens, tok.at[0, 0]),
                (ids, idt.at[0, 0]),
                (gate, gu.at[0, :, pl.ds(0, HID)]),
                (up, gu.at[0, :, pl.ds(HID, HID)]),
                (sgate, sgw),
                (sup, suw),
                (sdown, sdw),
                (down, dn.at[:, pl.ds(0, HID)]),
            )
        )
    ]
    for copy in local:
        copy.start()

    barrier = pltpu.get_barrier_semaphore()
    for device in (*to_x, *to_y, *to_z, partner):
        pl.semaphore_signal(barrier, inc=1, device_id=device, device_id_type=MESH)
    pl.semaphore_wait(barrier, 7)

    links = Links(send_sem, recv_sem)
    add, send, arrive = links.add, links.send, links.arrive

    near = (1, 3)
    lo, hi = pl.ds(0, HALF_T), pl.ds(HALF_T, HALF_T)
    for way in range(2):
        add(("xt", way), tok.at[0, 0], tok.at[near[way], 0], to_x[way])
        add(("xi", way), idt.at[0, 0], idt.at[near[way], 0], to_x[way])
        part = (lo, hi)[way]
        add(("xf", way), tok.at[near[way], 0, part], tok.at[2, 0, part], to_x[way])
    add(("xif",), idt.at[1, 0], idt.at[2, 0], to_x[0])
    for rx in range(XN):
        add(("ct", rx), tok.at[rx, 0], tok.at[rx, 1], partner)
        add(("ci", rx), idt.at[rx, 0], idt.at[rx, 1], partner)

    for b in range(BLOCKS):
        span = pl.ds(b * CAP, CAP)
        for way in range(2):
            add(("yr", way, b), rows.at[0, span], rows.at[near[way], span], to_y[way])
        way = b % 2
        add(("yf", b), rows.at[near[way], span], rows.at[2, span], to_y[way])

    def z_slot(way, hop):
        return hop if way == 0 else (ZN - hop) % ZN

    lanes = (pl.ds(0, HID), pl.ds(HID, HID))
    for hop in range(1, 5):
        for way in range(2):
            src, dst = z_slot(way, hop - 1), z_slot(way, hop)
            for which in range(2):
                if hop < 4 or which == way:
                    add(("zw", way, hop, which), gu.at[src, :, lanes[which]], gu.at[dst, :, lanes[which]], to_z[way])
            for c in range(NC):
                if hop < 4 or c % 2 == way:
                    span = pl.ds(c * CW, CW)
                    add(
                        ("zd", way, hop, c),
                        dn.at[span, pl.ds(src * HID, HID)],
                        dn.at[span, pl.ds(dst * HID, HID)],
                        to_z[way],
                    )

    for c in range(NC):
        for way in range(2):
            add(("y1", way, c), ys1.at[c, way], yr1.at[c, way], to_y[way])
            add(("y2", way, c), ys2.at[c, way], yr2.at[c, way], to_y[way])
            add(("y3", way, c), ys3.at[c, way], yr3.at[c, way], to_y[way])
            add(("x1", way, c), xs1.at[c, way], xr1.at[c, way], to_x[way])
            add(("x2", way, c), xs2.at[c, way], xr2.at[c, way], to_x[way])
            add(("x3", way, c), xs3.at[c, way], xr3.at[c, way], to_x[way])
        add(("cr", c), csend.at[c], crecv.at[c], partner)
    assert len(links.copies) <= COPIES

    row_iota = lax.broadcasted_iota(jnp.int32, (TOK, TOK), 0)
    lane_iota = lax.broadcasted_iota(jnp.int32, (TOK, TOK), 1)
    eye = jnp.where(row_iota == lane_iota, 1.0, 0.0).astype(BF16)
    earlier = jnp.where(lane_iota < row_iota, 1.0, 0.0).astype(BF16)
    lane = lane_iota.astype(F32)
    lane8 = lax.broadcasted_iota(jnp.int32, (TOK, BLOCKS), 1).astype(F32)
    mine = e.astype(F32)

    def take_block(b):
        rx, cc = b // 2, b % 2
        wide = tok[rx, cc].astype(F32)
        mean_square = jnp.mean(wide * wide, axis=-1, keepdims=True)
        n = (wide * lax.rsqrt(mean_square + 1e-06) * gain[...]).astype(BF16)
        xn[pl.ds(b * TOK, TOK), :] = n
        logits = dot(n, router[...])
        columns = lax.dot_general(eye, idt[rx, cc].astype(BF16), NT, preferred_element_type=F32)
        id0, id1 = columns[:, 0:1], columns[:, 1:2]
        l0 = jnp.sum(jnp.where(lane8 == id0, logits, 0.0), axis=-1, keepdims=True)
        l1 = jnp.sum(jnp.where(lane8 == id1, logits, 0.0), axis=-1, keepdims=True)
        w0 = jax.nn.sigmoid(l0 - l1)
        wcol[b] = jnp.where(id0 == mine, w0, 0.0) + jnp.where(id1 == mine, 1.0 - w0, 0.0)
        named = jnp.where(id0 == mine, 1.0, 0.0) + jnp.where(id1 == mine, 1.0, 0.0)
        named = jnp.broadcast_to(named, (TOK, TOK))
        slot = dot(earlier, named.astype(BF16))
        chosen = jnp.where(slot == lane, named, 0.0)
        sel[b] = chosen.astype(BF16)
        table = jnp.transpose(chosen)[0:CAP, :].astype(BF16)
        rows[0, pl.ds(b * CAP, CAP), :] = dot(table, n).astype(BF16)
        gcol[b] = jax.nn.sigmoid(
            jnp.sum(n.astype(F32) * gate_vector[...], axis=-1, keepdims=True)
        )
        for way in range(2):
            send("yr", way, b)

    def shared_pair(p):
        a = xn[pl.ds(p * 2 * TOK, 2 * TOK), :]
        hidden = silu_mul(dot(a, sgw[...]), dot(a, suw[...]))
        part = dot(hidden, sdw[...])
        for k in range(2):
            b = 2 * p + k
            shared[b] = part[k * TOK : (k + 1) * TOK] * gcol[b]

    def gate_up(s):
        @pl.loop(0, YN)
        def _(r):
            both = dot(rows[r], gu[s])
            hid[r, :, pl.ds(s * HID, HID)] = silu_mul(both[:, :HID], both[:, HID:])

    def down_out(r, c):
        return lax.dot_general(
            hid[r], dn[pl.ds(c * CW, CW), :], NT, preferred_element_type=F32
        )

    def forward_weights(hop, which):
        for way in range(2):
            if ("zw", way, hop, which) in links.copies:
                arrive("zw", way, hop, which)
                if ("zw", way, hop + 1, which) in links.copies:
                    send("zw", way, hop + 1, which)

    def forward_rows(b):
        way = b % 2
        arrive("yr", way, b)
        send("yf", b)

    def down_round(r):
        for hop in range(1, 5):
            c = r - hop + 1
            if 0 <= c < NC:
                for way in range(2):
                    if ("zd", way, hop, c) in links.copies:
                        if hop > 1:
                            arrive("zd", way, hop - 1, c)
                        send("zd", way, hop, c)

    def out_chunk(c):
        for hop in range(1, 5):
            for way in range(2):
                if ("zd", way, hop, c) in links.copies:
                    arrive("zd", way, hop, c)
        far = down_out(2, c)
        ys1[c, 0] = far[:HALF_R].astype(BF16)
        ys1[c, 1] = far[HALF_R:].astype(BF16)
        send("y1", 0, c)
        send("y1", 1, c)
        after = down_out(3, c)
        ys2[c, 0] = after[HALF_R:].astype(BF16)
        send("y2", 0, c)
        ymerge[c, 0] = after[:HALF_R]
        before = down_out(1, c)
        ys2[c, 1] = before[:HALF_R].astype(BF16)
        send("y2", 1, c)
        ymerge[c, 1] = before[HALF_R:]
        yown[c] = down_out(0, c)

    def y_merge(c):
        for way in range(2):
            arrive("y1", way, c)
            ys3[c, way] = (ymerge[c, way] + yr1[c, way].astype(F32)).astype(BF16)
            send("y3", way, c)

    def combine(c):
        for way in range(2):
            arrive("y2", way, c)
        for way in range(2):
            arrive("y3", way, c)
        own = yown[c]
        top = own[:HALF_R] + yr3[c, 0].astype(F32) + yr2[c, 1].astype(F32)
        bottom = own[HALF_R:] + yr2[c, 0].astype(F32) + yr3[c, 1].astype(F32)
        per_half = HALF_R // CAP
        halves = (top.astype(BF16), bottom.astype(BF16))
        for cc in (1, 0):
            for rx in range(XN):
                b = rx * 2 + cc
                k = b % per_half
                chosen = halves[b // per_half][k * CAP : (k + 1) * CAP]
                part = dot(sel[b][:, :CAP], chosen) * wcol[b] + shared[b, :, pl.ds(c * CW, CW)]
                if cc == 1:
                    csend[c, rx] = part.astype(BF16)
                else:
                    cown[c, rx] = part
            if cc == 1:
                send("cr", c)

    def core_merge(c):
        arrive("cr", c)
        far = cown[c, 2] + crecv[c, 2].astype(F32)
        xs1[c, 0] = far[:HALF_T].astype(BF16)
        xs1[c, 1] = far[HALF_T:].astype(BF16)
        send("x1", 0, c)
        send("x1", 1, c)
        after = cown[c, 3] + crecv[c, 3].astype(F32)
        xs2[c, 0] = after[HALF_T:].astype(BF16)
        send("x2", 0, c)
        xmerge[c, 0] = after[:HALF_T]
        before = cown[c, 1] + crecv[c, 1].astype(F32)
        xs2[c, 1] = before[:HALF_T].astype(BF16)
        send("x2", 1, c)
        xmerge[c, 1] = before[HALF_T:]

    def x_merge(c):
        for way in range(2):
            arrive("x1", way, c)
            xs3[c, way] = (xmerge[c, way] + xr1[c, way].astype(F32)).astype(BF16)
            send("x3", way, c)

    def finish_chunk(c):
        for way in range(2):
            arrive("x2", way, c)
        for way in range(2):
            arrive("x3", way, c)
        own = cown[c, 0] + crecv[c, 0].astype(F32)
        columns = pl.ds(c * CW, CW)
        out[pl.ds(0, HALF_T), columns] = (
            own[:HALF_T] + xr3[c, 0].astype(F32) + xr2[c, 1].astype(F32)
        ).astype(BF16)
        out[pl.ds(HALF_T, HALF_T), columns] = (
            own[HALF_T:] + xr2[c, 0].astype(F32) + xr3[c, 1].astype(F32)
        ).astype(BF16)

    local[0].wait()
    local[1].wait()
    for way in range(2):
        send("xi", way)
        send("xt", way)
    send("ci", 0)
    send("ct", 0)
    local[2].wait()
    for way in range(2):
        send("zw", way, 1, 0)
    local[3].wait()
    for way in range(2):
        send("zw", way, 1, 1)

    take_block(0)
    arrive("ci", 0)
    arrive("ct", 0)
    take_block(1)
    for k in (4, 5, 6):
        local[k].wait()
    shared_pair(0)
    local[7].wait()

    for way in range(2):
        rx = near[way]
        arrive("xi", way)
        if way == 0:
            send("xif")
        send("ci", rx)
        arrive("xt", way)
        send("xf", way)
        send("ct", rx)
    forward_rows(0)
    take_block(2)
    forward_weights(1, 0)
    take_block(6)
    forward_rows(1)
    for rx in (1, 3):
        arrive("ci", rx)
        arrive("ct", rx)
        take_block(rx * 2 + 1)
    forward_weights(1, 1)
    arrive("xif")
    send("ci", 2)
    arrive("xf", 0)
    arrive("xf", 1)
    send("ct", 2)
    take_block(4)
    forward_rows(2)
    arrive("ci", 2)
    arrive("ct", 2)
    take_block(5)
    forward_rows(6)
    shared_pair(1)
    forward_weights(2, 0)
    forward_rows(3)
    forward_rows(7)
    shared_pair(3)
    forward_weights(2, 1)
    forward_rows(4)
    down_round(0)
    forward_rows(5)
    shared_pair(2)
    for b in range(BLOCKS):
        for way in range(2):
            arrive("yr", way, b)
        arrive("yf", b)
    gate_up(0)
    forward_weights(3, 0)
    gate_up(1)
    gate_up(7)
    gate_up(2)
    gate_up(6)
    forward_weights(3, 1)
    down_round(1)
    gate_up(3)
    gate_up(5)
    down_round(2)
    forward_weights(4, 0)
    forward_weights(4, 1)
    down_round(3)
    gate_up(4)

    for c in range(NC):
        out_chunk(c)
        if c + 4 < NC + 3:
            down_round(c + 4)
        y_merge(c)
        if c > 0:
            combine(c - 1)
            core_merge(c - 1)
        if c > 1:
            x_merge(c - 2)
            finish_chunk(c - 2)
    x_merge(NC - 2)
    combine(NC - 1)
    core_merge(NC - 1)
    finish_chunk(NC - 2)
    x_merge(NC - 1)
    finish_chunk(NC - 1)
    links.finish()


def body(
    tokens,
    norm_gain,
    router_weight,
    shared_gate_vector,
    expert_ids,
    gate_weight,
    up_weight,
    down_weight,
    shared_gate_weight,
    shared_up_weight,
    shared_down_weight,
):
    ids = jnp.pad(expert_ids.T.astype(F32), ((0, 6), (0, 0)))
    anywhere = pl.BlockSpec(memory_space=pl.ANY)
    inside = pl.BlockSpec(memory_space=pltpu.VMEM)
    vmem = pltpu.VMEM
    return pl.pallas_call(
        layer_kernel,
        out_shape=jax.ShapeDtypeStruct((TOK, D), BF16),
        in_specs=[anywhere, anywhere, inside, inside, inside] + [anywhere] * 6,
        out_specs=inside,
        scratch_shapes=[
            vmem((XN, CN, TOK, D), BF16),
            vmem((XN, CN, 8, TOK), F32),
            vmem((BLOCKS * TOK, D), BF16),
            vmem((BLOCKS, TOK, TOK), BF16),
            vmem((BLOCKS, TOK, 1), F32),
            vmem((BLOCKS, TOK, 1), F32),
            vmem((YN, ROWS, D), BF16),
            vmem((ZN, D, 2 * HID), BF16),
            vmem((D, ZN * HID), BF16),
            vmem((YN, ROWS, ZN * HID), BF16),
            vmem((D, SHID), BF16),
            vmem((D, SHID), BF16),
            vmem((SHID, D), BF16),
            vmem((BLOCKS, TOK, D), F32),
            vmem((NC, ROWS, CW), F32),
            vmem((NC, 2, HALF_R, CW), F32),
        ]
        + [vmem((NC, 2, HALF_R, CW), BF16)] * 6
        + [vmem((NC, XN, TOK, CW), F32)]
        + [vmem((NC, XN, TOK, CW), BF16)] * 2
        + [vmem((NC, 2, HALF_T, CW), F32)]
        + [vmem((NC, 2, HALF_T, CW), BF16)] * 6
        + [
            pltpu.SemaphoreType.DMA((8,)),
            pltpu.SemaphoreType.DMA((COPIES,)),
            pltpu.SemaphoreType.DMA((COPIES,)),
        ],
        compiler_params=pltpu.CompilerParams(
            collective_id=0, has_side_effects=True, vmem_limit_bytes=60 * 1024 * 1024
        ),
        name="moe_layer",
    )(
        tokens,
        ids,
        norm_gain.reshape(1, D),
        router_weight,
        shared_gate_vector.reshape(1, D),
        gate_weight.reshape(D, HID),
        up_weight.reshape(D, HID),
        down_weight.reshape(D, HID),
        shared_gate_weight,
        shared_up_weight,
        shared_down_weight,
    )


def solution(mesh):
    return jax.shard_map(
        body,
        mesh=mesh,
        in_specs=(
            P(("expert", "dp"), None),
            P(),
            P(),
            P(),
            P(("expert", "dp"), None),
            P("expert", None, "dp"),
            P("expert", None, "dp"),
            P("expert", None, "dp"),
            P(None, "expert"),
            P(None, "expert"),
            P("expert", None),
        ),
        out_specs=P(("expert", "dp"), None),
        check_vma=False,
    )
```

```python
import math

import jax
import jax.numpy as jnp
from jax import lax
from jax.experimental import pallas as pl
from jax.experimental.pallas import tpu as pltpu
from jax.sharding import PartitionSpec as P

MESH = pl.DeviceIdType.MESH
BF16 = jnp.bfloat16
F32 = jnp.float32

XN, CN, YN, ZN = 4, 2, 4, 8
TOK = 128
D = 1024
HID = 128
SHID = 512
CAP = 48
BLOCKS = XN * CN
ROWS = BLOCKS * CAP
WIDTHS = (128, 256, 256, 256, 128)
NC = len(WIDTHS)
COLUMNS = tuple(pl.ds(sum(WIDTHS[:c]), WIDTHS[c]) for c in range(NC))
OPP, MATE, SWAP, OWN = range(YN)
HALF_R = ROWS // 2
HALF_T = TOK // 2
COPIES = 256
OPENED_N = ("zn_{0}_1_0", "zn_{0}_3_{0}", "zn_own_1", "zn_{0}_2_0", "d_{0}_2_2")
OPENED_F = ("zf_own_1", "zf_{0}_1_0", "zf_{0}_3_{0}", "zf_own_1", "zf_{0}_3_{0}")

NT = (((1,), (1,)), ((), ()))


def dot(a, b):
    return jnp.dot(a, b, preferred_element_type=F32)


class Links:
    def __init__(self, send_sem, recv_sem):
        self.send_sem, self.recv_sem = send_sem, recv_sem
        self.copies, self.started, self.arrived, self.sizes = {}, set(), set(), {}

    def add(self, name, link, src, dst, device):
        k = len(self.copies)
        size = math.prod(src.shape) * src.dtype.itemsize
        self.sizes[name] = (link, size)
        self.copies[name] = pltpu.make_async_remote_copy(
            src_ref=src,
            dst_ref=dst,
            send_sem=self.send_sem.at[k],
            recv_sem=self.recv_sem.at[k],
            device_id=device,
            device_id_type=MESH,
        )

    def send(self, name, kind=None):
        assert (name, kind) not in self.started
        self.started.add((name, kind))
        self.copies[name].start()

    def arrive(self, name, kind=None):
        if (name, kind) not in self.arrived and (name, None) not in self.arrived:
            self.arrived.add((name, kind))
            with jax.named_scope("w_" + "_".join(map(str, name))):
                self.copies[name].wait_recv()


RATE = {"c": 600e3, "x": 46e3, "y": 46e3, "z": 92e3, "w": 92e3}
DELAY = {"c": 1.6, "x": 2.7, "y": 2.7, "z": 2.7, "w": 3.6}
LATE = {"ct": 3.0, "rm": 2.0, "rs": 2.0, "rf": 2.0, "rc": 2.0}


class Plan:
    def __init__(self, sizes):
        self.sizes = sizes
        self.tasks = {}

    def task(self, name, run, us, rank, needs=(), after=(), sends=(), kind=None):
        assert name not in self.tasks
        self.tasks[name] = (run, us, rank, tuple(needs), tuple(after), tuple(sends), kind)

    def order(self):
        now, done, arrival, lines = 0.0, set(), {}, {}
        left, steps = dict(self.tasks), []

        def kinds(copy, kind):
            along_z = self.sizes[copy][0][0] == "z"
            return (kind or "nf") if along_z else "-"

        def advance(until):
            nonlocal now
            while now < until:
                for link, lanes in lines.items():
                    busy = [q for q in lanes.values() if q]
                    for q in busy:
                        q[0][2] = RATE[link[0]] / len(busy)
                first = [q[0][1] / q[0][2] for lanes in lines.values() for q in lanes.values() if q]
                by = min([until - now] + first)
                now += by
                for link, lanes in lines.items():
                    for k, q in lanes.items():
                        if q:
                            q[0][1] -= by * q[0][2]
                            if q[0][1] < 1e-3:
                                arrival[q.pop(0)[0], k] = now + DELAY[link[0]]

        def next_event():
            soon = [t + late for (n, _), t in arrival.items() for late in (0.0, LATE.get(n[0], 0.0)) if t + late > now]
            for link, lanes in lines.items():
                busy = [q for q in lanes.values() if q]
                soon += [now + q[0][1] / (RATE[link[0]] / len(busy)) for q in busy]
            return min(soon)

        while left:
            ready = []
            for k, (name, (_, _, rank, needs, after, _, kind)) in enumerate(left.items()):
                if all(t in done for t in after) and all(
                    arrival.get((n, w), 1e9) + LATE.get(n[0], 0.0) <= now + 1e-6
                    for n in needs
                    for w in kinds(n, kind)
                ):
                    ready.append((rank, k, name))
            if not ready:
                advance(next_event())
                continue
            name = min(ready)[2]
            _, us, _, _, _, sends, kind = left.pop(name)
            steps.append((now, name))
            advance(now + us)
            done.add(name)
            for n in sends:
                link, size = self.sizes[n]
                for w in kinds(n, kind):
                    lines.setdefault(link, {}).setdefault(w, []).append([n, float(size), 1.0])
        self.end = now
        return steps


def silu_mul(g, u):
    return (g * jax.nn.sigmoid(g) * u).astype(BF16)


def layer_kernel(
    tokens, ids, gain, router, gate_vector, gate, up, down, sgate, sup, sdown, out,
    tok, idt, xn, sel, wcol, gcol, rows, frow, gu, dn, hid, sgw, suw, sdw,
    sown, ssend, srecv, pown, psend, precv, rrow, y1s, y2s, y3s, y1r, y2r, y3r,
    cown, xmerge, xs1, xs2, xs3, xr1, xr2, xr3,
    local_sem, send_sem, recv_sem,
):
    e, d = lax.axis_index("expert"), lax.axis_index("dp")
    x, core = lax.div(e, CN), lax.rem(e, CN)
    y, z = lax.div(d, ZN), lax.rem(d, ZN)
    role, odd = lax.div(y, 2), lax.rem(y, 2)
    mate_y = y + 1 - 2 * odd
    swap_y = lax.rem(y + 3 + 2 * odd, YN)
    native, foreign = core == role, core != role

    def step_x(by):
        return (lax.rem(x + by, XN) * CN + core, d)

    def step_z(by):
        return (e, y * ZN + lax.rem(z + by, ZN))

    to_x = (step_x(1), step_x(XN - 1))
    to_z = (step_z(1), step_z(ZN - 1))
    mate, swap = (e, mate_y * ZN + z), (e, swap_y * ZN + z)
    partner = (x * CN + (1 - core), d)
    cross = (x * CN + (1 - core), swap_y * ZN + z)

    first_lanes = pl.ds(0, HID)
    own_weights = (
        (gate, gu.at[0, :, first_lanes]),
        (up, gu.at[0, :, pl.ds(HID, HID)]),
        (down, dn.at[:, first_lanes]),
    )
    pairs = ((tokens, tok.at[0, 0]), (ids, idt.at[0]), *own_weights, (sgate, sgw), (sup, suw), (sdown, sdw))
    local = [pltpu.make_async_copy(src, dst, local_sem.at[i]) for i, (src, dst) in enumerate(pairs)]
    for i in (0, 1):
        local[i].start()

    @pl.when(native)
    def _():
        for i in (2, 3, 4):
            local[i].start()

    for i in (5, 6, 7):
        local[i].start()

    barrier = pltpu.get_barrier_semaphore()
    for device in (*to_x, *to_z, partner, mate, swap, cross):
        pl.semaphore_signal(barrier, inc=1, device_id=device, device_id_type=MESH)
    with jax.named_scope("meet"):
        pl.semaphore_wait(barrier, 8)

    links = Links(send_sem, recv_sem)
    add = links.add

    near = (1, 3)
    lo, hi = pl.ds(0, HALF_T), pl.ds(HALF_T, HALF_T)
    for way in range(2):
        add(("xt", way), f"x{way}", tok.at[0, 0], tok.at[near[way], 0], to_x[way])
        add(("xi", way), f"x{way}", idt.at[0], idt.at[near[way]], to_x[way])
        part = (lo, hi)[way]
        add(("xf", way), f"x{way}", tok.at[near[way], 0, part], tok.at[2, 0, part], to_x[way])
    add(("xif",), "x0", idt.at[1], idt.at[2], to_x[0])
    for rx in range(XN):
        add(("ct", rx), "c", tok.at[rx, 0], tok.at[rx, 1], partner)

    for rx in range(XN):
        span = pl.ds(rx * CAP, CAP)
        add(("rs", rx), "ys", frow.at[span], rows.at[SWAP, 0, span], swap)
        add(("rm", rx), "ym", rows.at[OWN, 0, span], rows.at[MATE, 0, span], mate)
        add(("rf", rx), "ym", rows.at[SWAP, 0, span], rows.at[OPP, 0, span], mate)
        for pos in range(YN):
            add(("rc", pos, rx), "c", rows.at[pos, 0, span], rows.at[pos, 1, span], partner)

    for k, (src, dst) in enumerate(own_weights):
        add(("w", k), "w", src, dst, cross)

    def z_slot(way, hop):
        return hop if way == 0 else (ZN - hop) % ZN

    lanes = (first_lanes, pl.ds(HID, HID))
    for hop in range(1, 5):
        for way in range(2):
            src, dst = z_slot(way, hop - 1), z_slot(way, hop)
            for which in range(2):
                if hop < 4 or which == way:
                    add(("zw", way, hop, which), f"z{way}", gu.at[src, :, lanes[which]], gu.at[dst, :, lanes[which]], to_z[way])
            for c in range(NC):
                if hop < 4 or c % 2 == way:
                    span = COLUMNS[c]
                    add(
                        ("zd", way, hop, c),
                        f"z{way}",
                        dn.at[span, pl.ds(src * HID, HID)],
                        dn.at[span, pl.ds(dst * HID, HID)],
                        to_z[way],
                    )

    for rx in range(XN):
        add(("sc", rx), "c", ssend.at[rx], srecv.at[rx], partner)
    for c in range(NC):
        cols = COLUMNS[c]
        add(("pf", c), "c", psend.at[OPP, :, cols], precv.at[OPP, :, cols], partner)
        rest = pl.ds(MATE, 3)
        add(("pn", c), "c", psend.at[rest, :, cols], precv.at[rest, :, cols], partner)
        add(("y1", c), "ym", y1s.at[:, cols], y1r.at[:, cols], mate)
        add(("y2", c), "ym", y2s.at[:, cols], y2r.at[:, cols], mate)
        add(("y3", c), "ys", y3s.at[:, cols], y3r.at[:, cols], swap)
        for way in range(2):
            add(("x1", way, c), f"x{way}", xs1.at[way, :, cols], xr1.at[way, :, cols], to_x[way])
            add(("x2", way, c), f"x{way}", xs2.at[way, :, cols], xr2.at[way, :, cols], to_x[way])
            add(("x3", way, c), f"x{way}", xs3.at[way, :, cols], xr3.at[way, :, cols], to_x[way])
    assert len(links.copies) <= COPIES

    row_iota = lax.broadcasted_iota(jnp.int32, (TOK, TOK), 0)
    lane_iota = lax.broadcasted_iota(jnp.int32, (TOK, TOK), 1)
    eye = jnp.where(row_iota == lane_iota, 1.0, 0.0).astype(BF16)
    earlier = jnp.where(lane_iota < row_iota, 1.0, 0.0).astype(BF16)
    lane = lane_iota.astype(F32)
    lane8 = lax.broadcasted_iota(jnp.int32, (TOK, BLOCKS), 1).astype(F32)
    experts = ((x * CN + role).astype(F32), (x * CN + 1 - role).astype(F32))
    plan = Plan(links.sizes)

    def step(us, rank, name, needs=(), after=(), sends=(), kind=None):
        def keep(run):
            plan.task(name, run, us, rank, needs, after, sends, kind)

        return keep

    def passing(rank, name, needs, sends, after=(), kind=None):
        plan.task(name, lambda: None, 0.03, rank, needs, after, sends, kind)

    @step(0.05, 0, "swap_weights", sends=[("w", k) for k in range(3)], kind="f")
    def _():
        pass

    @step(0.05, 0, "own_tokens", sends=[("xi", 0), ("xt", 0), ("xi", 1), ("xt", 1), ("ct", 0)])
    def _():
        local[0].wait()
        local[1].wait()

    for which in range(2):
        both_ways = [("zw", way, 1, which) for way in range(2)]

        @step(0.05, 1, f"zn_own_{which}", sends=both_ways, kind="n")
        def _(which=which):
            local[2 + which].wait()

        passing(0, f"zf_own_{which}", [("w", which)], both_ways, kind="f")

    @step(0.05, 3, "own_down_n", kind="n")
    def _():
        local[4].wait()

    passing(3, "own_down_f", [("w", 2)], [], kind="f")

    @step(0.05, 40, "own_shared")
    def _():
        for i in (5, 6, 7):
            local[i].wait()

    passing(1, "x_ids", [("xi", 0)], [("xif",)])
    for way in range(2):
        passing(2, f"x_tok_{way}", [("xt", way)], [("xf", way), ("ct", near[way])])
    passing(2, "x_far", [("xf", 0), ("xf", 1)], [("ct", 2)])

    def normed(rx, cc):
        wide = tok[rx, cc].astype(F32)
        mean_square = jnp.mean(wide * wide, axis=-1, keepdims=True)
        n = (wide * lax.rsqrt(mean_square + 1e-06) * gain[...]).astype(BF16)
        b = 2 * rx + cc
        xn[pl.ds(b * TOK, TOK), :] = n
        gcol[b] = jax.nn.sigmoid(
            jnp.sum(n.astype(F32) * gate_vector[...], axis=-1, keepdims=True)
        )
        return n

    def take_block(rx):
        needs = ([], [], [("xif",)], [("xi", 1)])[rx]
        after = ["own_tokens"] if rx == 0 else ["x_ids", ("", "x_tok_0", "x_far", "x_tok_1")[rx]]

        @step(1.1, 20, f"take_{rx}", needs, after, [("rs", rx), ("rm", rx), ("rc", OWN, rx)])
        def _():
            n = normed(rx, 0)
            logits = lax.dot_general(n, router[...], NT, preferred_element_type=F32)
            columns = lax.dot_general(
                eye, idt[rx].astype(F32).astype(BF16), NT, preferred_element_type=F32
            )
            id0, id1 = columns[:, 0:1], columns[:, 1:2]
            l0 = jnp.sum(jnp.where(lane8 == id0, logits, 0.0), axis=-1, keepdims=True)
            l1 = jnp.sum(jnp.where(lane8 == id1, logits, 0.0), axis=-1, keepdims=True)
            w0 = jax.nn.sigmoid(l0 - l1)
            span = pl.ds(rx * CAP, CAP)
            for k in (1, 0):
                is0, is1 = id0 == experts[k], id1 == experts[k]
                wcol[k, rx] = jnp.where(is0, w0, 0.0) + jnp.where(is1, 1.0 - w0, 0.0)
                named = jnp.where(is0, 1.0, 0.0) + jnp.where(is1, 1.0, 0.0)
                named = jnp.broadcast_to(named, (TOK, TOK))
                slot = dot(earlier, named.astype(BF16))
                chosen = jnp.where(slot == lane, named, 0.0)
                sel[k, rx] = chosen.astype(BF16)
                table = jnp.transpose(chosen)[0:CAP, :].astype(BF16)
                found = dot(table, n).astype(BF16)
                if k == 0:
                    rows[OWN, 0, span, :] = found
                else:
                    frow[span, :] = found

    def take_other(rx):
        @step(0.35, 35, f"other_{rx}", [("ct", rx)])
        def _():
            normed(rx, 1)

    def shared_pair(rx):
        @step(1.07, 50, f"shared_{rx}", [], ["own_shared", f"take_{rx}", f"other_{rx}"], [("sc", rx)])
        def _():
            a = xn[pl.ds(rx * 2 * TOK, 2 * TOK), :]
            hidden = silu_mul(dot(a, sgw[...]), dot(a, suw[...]))
            part = dot(hidden, sdw[...])
            sown[rx] = part[:TOK] * gcol[2 * rx]
            ssend[rx] = (part[TOK:] * gcol[2 * rx + 1]).astype(BF16)

    every_row = []
    for rx in range(XN):
        take_block(rx)
        take_other(rx)
        shared_pair(rx)
        passing(4, f"rows_mate_{rx}", [("rm", rx)], [("rc", MATE, rx)])
        passing(4, f"rows_swap_{rx}", [("rs", rx)], [("rf", rx), ("rc", SWAP, rx)])
        passing(4, f"rows_opp_{rx}", [("rf", rx)], [("rc", OPP, rx)])
        every_row += [("rc", pos, rx) for pos in range(YN)]
    rows_here = [f"rows_{k}_{rx}" for k in ("mate", "swap", "opp") for rx in range(XN)]

    of_slot = {s: [] for s in range(ZN)}
    for kind in "nf":
        of_slot[0] += [f"z{kind}_own_{which}" for which in range(2)]
        for hop in range(1, 5):
            for which in range(2):
                for way in range(2):
                    if ("zw", way, hop, which) in links.copies:
                        onward = [("zw", way, hop + 1, which)]
                        onward = [n for n in onward if n in links.copies]
                        name = f"z{kind}_{way}_{hop}_{which}"
                        passing(0, name, [("zw", way, hop, which)], onward, kind=kind)
                        of_slot[z_slot(way, hop)].append(name)
    for c in range(NC):
        for way in range(2):
            for kind, opened in (("n", OPENED_N), ("f", OPENED_F)):
                last = [f"own_down_{kind}", opened[c].format(way)]
                passing(1, f"d{kind}_{way}_1_{c}", [], [("zd", way, 1, c)], last, kind)
            for hop in range(2, 5):
                if ("zd", way, hop, c) in links.copies:
                    passing(1, f"d_{way}_{hop}_{c}", [("zd", way, hop - 1, c)], [("zd", way, hop, c)])

    def gate_up(s):
        @step(1.0, 30, f"gate_up_{s}", every_row, of_slot[s] + rows_here)
        def _():
            for k in range(YN):
                both = dot(rows[k].reshape(ROWS, D), gu[s])
                hid[pl.ds(k * ROWS, ROWS), pl.ds(s * HID, HID)] = silu_mul(both[:, :HID], both[:, HID:])

    for s in (0, 1, 7, 2, 6, 3, 5, 4):
        gate_up(s)
    hidden_done = [f"gate_up_{s}" for s in range(ZN)]

    def way_back(c):
        columns = COLUMNS[c]
        needs = [n for n in links.copies if n[0] == "zd" and n[3] == c]

        def down_out(first, many):
            h = hid[pl.ds(first * ROWS, many * ROWS), :]
            part = lax.dot_general(h, dn[columns, :], NT, preferred_element_type=F32)
            for k in range(many):
                pown[first + k, :, columns] = part[k * ROWS : k * ROWS + HALF_R]
                psend[first + k, :, columns] = part[k * ROWS + HALF_R : (k + 1) * ROWS].astype(BF16)

        def chip(pos):
            return pown[pos, :, columns] + precv[pos, :, columns].astype(F32)

        @step(0.6, 25, f"far_{c}", needs, hidden_done + ["own_down_n", "own_down_f"], [("pf", c)])
        def _():
            down_out(OPP, 1)

        @step(1.4, 25, f"near_{c}", [], [f"far_{c}"], [("pn", c)])
        def _():
            down_out(MATE, 3)

        @step(0.1, 9, f"opp_{c}", [("pf", c)], [f"near_{c}"], [("y1", c)])
        def _():
            y1s[:, columns] = chip(OPP).astype(BF16)

        @step(0.1, 9, f"mate_{c}", [("pn", c)], [f"near_{c}"], [("y2", c)])
        def _():
            y2s[:, columns] = chip(MATE).astype(BF16)

        @step(0.1, 8, f"swap_{c}", [("y1", c), ("pn", c)], [f"near_{c}"], [("y3", c)])
        def _():
            y3s[:, columns] = (chip(SWAP) + y1r[:, columns].astype(F32)).astype(BF16)

        @step(
            0.45, 8, f"combine_{c}",
            [("y2", c), ("y3", c), ("pn", c)] + [("sc", rx) for rx in range(XN)],
            [f"near_{c}"] + [f"shared_{rx}" for rx in range(XN)],
            [("x1", 0, c), ("x1", 1, c), ("x2", 0, c), ("x2", 1, c)],
        )
        def _():
            rrow[:, columns] = (chip(OWN) + y2r[:, columns].astype(F32)).astype(BF16)

            def part(rx):
                span = pl.ds(rx * CAP, CAP)
                here = dot(sel[0, rx][:, :CAP], rrow[span, columns]) * wcol[0, rx]
                there = dot(sel[1, rx][:, :CAP], y3r[span, columns]) * wcol[1, rx]
                return here + there + sown[rx, :, columns] + srecv[rx, :, columns].astype(F32)

            far = part(2)
            xs1[0, :, columns] = far[:HALF_T].astype(BF16)
            xs1[1, :, columns] = far[HALF_T:].astype(BF16)
            after = part(3)
            xs2[0, :, columns] = after[HALF_T:].astype(BF16)
            xmerge[0, :, columns] = after[:HALF_T]
            before = part(1)
            xs2[1, :, columns] = before[:HALF_T].astype(BF16)
            xmerge[1, :, columns] = before[HALF_T:]
            cown[:, columns] = part(0)

        def x_merge(way):
            @step(0.06, 7, f"x_merge_{way}_{c}", [("x1", way, c)], [f"combine_{c}"], [("x3", way, c)])
            def _():
                xs3[way, :, columns] = (
                    xmerge[way, :, columns] + xr1[way, :, columns].astype(F32)
                ).astype(BF16)

        x_merge(0)
        x_merge(1)

        @step(0.1, 12, f"finish_{c}", [(k, way, c) for k in ("x2", "x3") for way in range(2)], [f"combine_{c}"])
        def _():
            own = cown[:, columns]
            out[pl.ds(0, HALF_T), columns] = (
                own[:HALF_T] + xr3[0, :, columns].astype(F32) + xr2[1, :, columns].astype(F32)
            ).astype(BF16)
            out[pl.ds(HALF_T, HALF_T), columns] = (
                own[HALF_T:] + xr2[0, :, columns].astype(F32) + xr3[1, :, columns].astype(F32)
            ).astype(BF16)

    for c in range(NC):
        way_back(c)

    only = {"n": native, "f": foreign}
    for _, name in plan.order():
        run, _, _, needs, _, sends, kind = plan.tasks[name]

        def carry_out(run=run, needs=needs, sends=sends, name=name, kind=kind):
            for n in needs:
                links.arrive(n, kind)
            with jax.named_scope(name):
                run()
            for n in sends:
                links.send(n, kind)

        if kind is None:
            carry_out()
        else:
            pl.when(only[kind])(carry_out)
    for name in links.copies:
        whole = ({None}, {"f"} if name[0] == "w" else {"n", "f"})
        assert {k for m, k in links.started if m == name} in whole
        assert {k for m, k in links.arrived if m == name} in whole
    with jax.named_scope("finish"):

        @pl.when(foreign)
        def _():
            for k in range(3):
                links.copies["w", k].wait_send()

        for name, copy in links.copies.items():
            if name[0] != "w":
                copy.wait_send()


def body(
    tokens,
    norm_gain,
    router_weight,
    shared_gate_vector,
    expert_ids,
    gate_weight,
    up_weight,
    down_weight,
    shared_gate_weight,
    shared_up_weight,
    shared_down_weight,
):
    anywhere = pl.BlockSpec(memory_space=pl.ANY)
    inside = pl.BlockSpec(memory_space=pltpu.VMEM)
    vmem = pltpu.VMEM
    return pl.pallas_call(
        layer_kernel,
        out_shape=jax.ShapeDtypeStruct((TOK, D), BF16),
        in_specs=[anywhere, anywhere, inside, inside, inside] + [anywhere] * 6,
        out_specs=inside,
        scratch_shapes=[
            vmem((XN, CN, TOK, D), BF16),
            vmem((XN, 2, TOK), jnp.int32),
            vmem((BLOCKS * TOK, D), BF16),
            vmem((2, XN, TOK, TOK), BF16),
            vmem((2, XN, TOK, 1), F32),
            vmem((BLOCKS, TOK, 1), F32),
            vmem((YN, 2, HALF_R, D), BF16),
            vmem((HALF_R, D), BF16),
            vmem((ZN, D, 2 * HID), BF16),
            vmem((D, ZN * HID), BF16),
            vmem((YN * ROWS, ZN * HID), BF16),
            vmem((D, SHID), BF16),
            vmem((D, SHID), BF16),
            vmem((SHID, D), BF16),
            vmem((XN, TOK, D), F32),
            vmem((XN, TOK, D), BF16),
            vmem((XN, TOK, D), BF16),
            vmem((YN, HALF_R, D), F32),
            vmem((YN, HALF_R, D), BF16),
            vmem((YN, HALF_R, D), BF16),
        ]
        + [vmem((HALF_R, D), BF16)] * 7
        + [vmem((TOK, D), F32), vmem((2, HALF_T, D), F32)]
        + [vmem((2, HALF_T, D), BF16)] * 6
        + [
            pltpu.SemaphoreType.DMA((8,)),
            pltpu.SemaphoreType.DMA((COPIES,)),
            pltpu.SemaphoreType.DMA((COPIES,)),
        ],
        compiler_params=pltpu.CompilerParams(
            collective_id=0, has_side_effects=True, vmem_limit_bytes=60 * 1024 * 1024
        ),
        name="moe_layer",
    )(
        tokens,
        expert_ids.T,
        norm_gain.reshape(1, D),
        router_weight.T,
        shared_gate_vector.reshape(1, D),
        gate_weight.reshape(D, HID),
        up_weight.reshape(D, HID),
        down_weight.reshape(D, HID),
        shared_gate_weight,
        shared_up_weight,
        shared_down_weight,
    )


def solution(mesh):
    return jax.shard_map(
        body,
        mesh=mesh,
        in_specs=(
            P(("expert", "dp"), None),
            P(),
            P(),
            P(),
            P(("expert", "dp"), None),
            P("expert", None, "dp"),
            P("expert", None, "dp"),
            P("expert", None, "dp"),
            P(None, "expert"),
            P(None, "expert"),
            P("expert", None),
        ),
        out_specs=P(("expert", "dp"), None),
        check_vma=False,
    )
```

```python
import jax
import jax.numpy as jnp
from jax import lax
from jax.experimental import pallas as pl
from jax.experimental.pallas import tpu as pltpu
from jax.sharding import PartitionSpec as P

MESH = pl.DeviceIdType.MESH
BF16 = jnp.bfloat16
F32 = jnp.float32

XN, CN, YN, ZN = 4, 2, 4, 8
TOK = 128
D = 1024
HID = 128
SHID = 512
CAP = 48
BLOCKS = XN * CN
ROWS = BLOCKS * CAP
WIDTHS = (256, 256, 256, 256)
NC = len(WIDTHS)
COLUMNS = tuple(pl.ds(sum(WIDTHS[:c]), WIDTHS[c]) for c in range(NC))
PARTS = [(columns,) for columns in COLUMNS[:-1]]
PARTS.append(tuple(pl.ds(D - WIDTHS[-1] + at, WIDTHS[-1] // 2) for at in (0, WIDTHS[-1] // 2)))
OTHERS = pl.ds(WIDTHS[0], D - WIDTHS[0])
OPP, MATE, SWAP, OWN = range(YN)
HALF_R = ROWS // 2
HALF_T = TOK // 2
COPIES = 256

NT = (((1,), (1,)), ((), ()))


def dot(a, b):
    return jnp.dot(a, b, preferred_element_type=F32)


class Links:
    def __init__(self, send_sem, recv_sem):
        self.send_sem, self.recv_sem = send_sem, recv_sem
        self.copies, self.started, self.arrived = {}, set(), set()

    def add(self, name, link, src, dst, device):
        k = len(self.copies)
        self.copies[name] = pltpu.make_async_remote_copy(
            src_ref=src,
            dst_ref=dst,
            send_sem=self.send_sem.at[k],
            recv_sem=self.recv_sem.at[k],
            device_id=device,
            device_id_type=MESH,
        )

    def send(self, name, kind=None):
        assert (name, kind) not in self.started
        self.started.add((name, kind))
        self.copies[name].start()

    def arrive(self, name, kind=None):
        if (name, kind) not in self.arrived and (name, None) not in self.arrived:
            self.arrived.add((name, kind))
            with jax.named_scope("w_" + "_".join(map(str, name))):
                self.copies[name].wait_recv()


STEPS = (
    5, 0, 3, 2, 7, 67, 98, 4, 10, 6, 42, 8, 68, 40, 15, 12, 11, 13, 33, 41, 73, 76, 90, 1, 53, 19, 69, 55, 54, 72, 14,
    46, 56, 16, 27, 85, 39, 9, 81, 99, 57, 18, 77, 22, 37, 21, 45, 17, 20, 44, 86, 70, 31, 58, 30, 80, 59, 25, 74, 61,
    32, 34, 28, 38, 60, 43, 48, 82, 36, 78, 87, 24, 26, 23, 35, 75, 107, 71, 50, 91, 47, 83, 106, 105, 63, 62, 64,
    109, 103, 94, 49, 108, 65, 100, 95, 92, 104, 88, 79, 84, 52, 51, 66, 110, 111, 96, 101, 112, 89, 93, 113, 120,
    114, 97, 102, 121, 122, 129, 130, 131, 115, 123, 138, 139, 147, 124, 140, 29, 133, 132, 116, 148, 149, 141, 125,
    142, 117, 118, 134, 150, 143, 119, 127, 136, 126, 135, 151, 152, 144, 145, 128, 153, 137, 146,
)


class Plan:
    def __init__(self):
        self.tasks = {}

    def task(self, name, run, us, rank, needs=(), after=(), sends=(), kind=None):
        assert name not in self.tasks
        self.tasks[name] = (run, us, rank, tuple(needs), tuple(after), tuple(sends), kind)

    def order(self):
        names = list(self.tasks)
        assert sorted(STEPS) == list(range(len(names)))
        done = set()
        for name in (names[k] for k in STEPS):
            assert done.issuperset(self.tasks[name][4])
            done.add(name)
            yield name


def silu_mul(g, u):
    return (g * jax.nn.sigmoid(g) * u).astype(BF16)


def layer_kernel(
    tokens, ids, gain, router, gate_vector, gate, up, down, sgate, sup, sdown, out,
    tok, idt, xn, sel, wcol, gcol, rows, frow, gu, dn, hid, sgw, suw, sdw,
    sown, ssend, srecv, pown, psend, precv, rrow, y1s, y2s, y3s, y1r, y2r, y3r,
    cown, xmerge, xs1, xs2, xs3, xr1, xr2, xr3, aside,
    local_sem, send_sem, recv_sem,
):
    e, d = lax.axis_index("expert"), lax.axis_index("dp")
    x, core = lax.div(e, CN), lax.rem(e, CN)
    y, z = lax.div(d, ZN), lax.rem(d, ZN)
    role, odd = lax.div(y, 2), lax.rem(y, 2)
    mate_y = y + 1 - 2 * odd
    swap_y = lax.rem(y + 3 + 2 * odd, YN)
    native, foreign = core == role, core != role

    def step_x(by):
        return (lax.rem(x + by, XN) * CN + core, d)

    def step_z(by):
        return (e, y * ZN + lax.rem(z + by, ZN))

    to_x = (step_x(1), step_x(XN - 1))
    to_z = (step_z(1), step_z(ZN - 1))
    mate, swap = (e, mate_y * ZN + z), (e, swap_y * ZN + z)
    partner = (x * CN + (1 - core), d)
    cross = (x * CN + (1 - core), swap_y * ZN + z)

    first_lanes = pl.ds(0, HID)
    own_weights = (
        (gate, gu.at[0, :, first_lanes]),
        (up, gu.at[0, :, pl.ds(HID, HID)]),
        (down.at[COLUMNS[0]], dn.at[COLUMNS[0], first_lanes]),
        (down.at[OTHERS], dn.at[OTHERS, first_lanes]),
    )
    pairs = ((tokens, tok.at[0, 0]), (ids, idt.at[0]), *own_weights, (sgate, sgw), (sup, suw), (sdown, sdw))
    local = [pltpu.make_async_copy(src, dst, local_sem.at[i]) for i, (src, dst) in enumerate(pairs)]
    for i in (0, 1):
        local[i].start()

    given = ((gate, aside.at[0]), (up, aside.at[1]), (down, aside.at[2]))
    lent = [pltpu.make_async_copy(src, dst, local_sem.at[2 + i]) for i, (src, dst) in enumerate(given)]

    @pl.when(native)
    def _():
        for i in (2, 3, 4, 5):
            local[i].start()

    @pl.when(foreign)
    def _():
        for copy in lent:
            copy.start()

    for i in (6, 7, 8):
        local[i].start()

    barrier = pltpu.get_barrier_semaphore()
    for device in (*to_x, *to_z, partner, mate, swap, cross):
        pl.semaphore_signal(barrier, inc=1, device_id=device, device_id_type=MESH)
    with jax.named_scope("meet"):
        pl.semaphore_wait(barrier, 8)

    links = Links(send_sem, recv_sem)
    add = links.add

    near = (1, 3)
    lo, hi = pl.ds(0, HALF_T), pl.ds(HALF_T, HALF_T)
    for way in range(2):
        add(("xt", way), f"x{way}", tok.at[0, 0], tok.at[near[way], 0], to_x[way])
        add(("xi", way), f"x{way}", idt.at[0], idt.at[near[way]], to_x[way])
        part = (lo, hi)[way]
        add(("xf", way), f"x{way}", tok.at[near[way], 0, part], tok.at[2, 0, part], to_x[way])
    add(("xif",), "x0", idt.at[1], idt.at[2], to_x[0])
    for rx in range(XN):
        add(("ct", rx), "c", tok.at[rx, 0], tok.at[rx, 1], partner)

    for rx in range(XN):
        span = pl.ds(rx * CAP, CAP)
        add(("rs", rx), "s", frow.at[span], rows.at[SWAP, 0, span], swap)
        add(("rm", rx), "y", rows.at[OWN, 0, span], rows.at[MATE, 0, span], mate)
        add(("rf", rx), "y", rows.at[SWAP, 0, span], rows.at[OPP, 0, span], mate)
        for pos in range(YN):
            add(("rc", pos, rx), "c", rows.at[pos, 0, span], rows.at[pos, 1, span], partner)

    sources = (aside.at[0], aside.at[1], aside.at[2, COLUMNS[0]], aside.at[2, OTHERS])
    for k, (src, (_, dst)) in enumerate(zip(sources, own_weights)):
        add(("w", k), "s", src, dst, cross)

    def z_slot(way, hop):
        return hop if way == 0 else (ZN - hop) % ZN

    lanes = (first_lanes, pl.ds(HID, HID))
    for hop in range(1, 5):
        for way in range(2):
            src, dst = z_slot(way, hop - 1), z_slot(way, hop)
            for which in range(2):
                if hop < 4 or which == way:
                    add(("zw", way, hop, which), f"z{way}", gu.at[src, :, lanes[which]], gu.at[dst, :, lanes[which]], to_z[way])
            for c in range(NC):
                if hop < 4 or c % 2 == way:
                    span = COLUMNS[c]
                    add(
                        ("zd", way, hop, c),
                        f"z{way}",
                        dn.at[span, pl.ds(src * HID, HID)],
                        dn.at[span, pl.ds(dst * HID, HID)],
                        to_z[way],
                    )

    for rx in range(XN):
        add(("sc", rx), "c", ssend.at[rx], srecv.at[rx], partner)
    for c in range(NC):
        cols = COLUMNS[c]
        add(("pf", c), "c", psend.at[OPP, :, cols], precv.at[OPP, :, cols], partner)
        rest = pl.ds(MATE, 3)
        add(("pn", c), "c", psend.at[rest, :, cols], precv.at[rest, :, cols], partner)
        for p, cols in enumerate(PARTS[c]):
            add(("y1", c, p), "y", y1s.at[:, cols], y1r.at[:, cols], mate)
            add(("y2", c, p), "y", y2s.at[:, cols], y2r.at[:, cols], mate)
            add(("y3", c, p), "s", y3s.at[:, cols], y3r.at[:, cols], swap)
            for way in range(2):
                add(("x1", way, c, p), f"x{way}", xs1.at[way, :, cols], xr1.at[way, :, cols], to_x[way])
                add(("x2", way, c, p), f"x{way}", xs2.at[way, :, cols], xr2.at[way, :, cols], to_x[way])
                add(("x3", way, c, p), f"x{way}", xs3.at[way, :, cols], xr3.at[way, :, cols], to_x[way])
    assert len(links.copies) <= COPIES

    row_iota = lax.broadcasted_iota(jnp.int32, (TOK, TOK), 0)
    lane_iota = lax.broadcasted_iota(jnp.int32, (TOK, TOK), 1)
    eye = jnp.where(row_iota == lane_iota, 1.0, 0.0).astype(BF16)
    earlier = jnp.where(lane_iota < row_iota, 1.0, 0.0).astype(BF16)
    lane = lane_iota.astype(F32)
    lane8 = lax.broadcasted_iota(jnp.int32, (TOK, BLOCKS), 1).astype(F32)
    experts = ((x * CN + role).astype(F32), (x * CN + 1 - role).astype(F32))
    plan = Plan()

    def step(us, rank, name, needs=(), after=(), sends=(), kind=None):
        def keep(run):
            plan.task(name, run, us, rank, needs, after, sends, kind)

        return keep

    def passing(rank, name, needs, sends, after=(), kind=None):
        plan.task(name, lambda: None, 0.03, rank, needs, after, sends, kind)

    @step(0.03, 0, "swap_weights", sends=[("w", 0), ("w", 1), ("w", 2)], kind="f")
    def _():
        for copy in lent:
            copy.wait()

    passing(0, "swap_down", [], [("w", 3)], ["take_3"], "f")

    @step(0.05, 0, "own_tokens", sends=[("xi", 0), ("xt", 0), ("xi", 1), ("xt", 1), ("ct", 0)])
    def _():
        local[0].wait()
        local[1].wait()

    for which in range(2):
        both_ways = [("zw", way, 1, which) for way in range(2)]

        @step(0.05, 1, f"zn_own_{which}", sends=both_ways, kind="n")
        def _(which=which):
            local[2 + which].wait()

        passing(0, f"zf_own_{which}", [("w", which)], both_ways, kind="f")

    @step(0.05, 3, "own_down_n", kind="n")
    def _():
        local[4].wait()
        local[5].wait()

    passing(1, "own_down_first", [("w", 2)], [], kind="f")
    passing(3, "own_down_f", [("w", 3)], [], ["own_down_first"], "f")

    @step(0.05, 40, "own_shared")
    def _():
        for i in (6, 7, 8):
            local[i].wait()

    passing(1, "x_ids", [("xi", 0)], [("xif",)])
    for way in range(2):
        passing(2, f"x_tok_{way}", [("xt", way)], [("xf", way), ("ct", near[way])])
    passing(2, "x_far", [("xf", 0), ("xf", 1)], [("ct", 2)])

    def normed(rx, cc):
        wide = tok[rx, cc].astype(F32)
        mean_square = jnp.mean(wide * wide, axis=-1, keepdims=True)
        n = (wide * lax.rsqrt(mean_square + 1e-06) * gain[...]).astype(BF16)
        b = 2 * rx + cc
        xn[pl.ds(b * TOK, TOK), :] = n
        gcol[b] = jax.nn.sigmoid(
            jnp.sum(n.astype(F32) * gate_vector[...], axis=-1, keepdims=True)
        )
        return n

    def take_block(rx):
        needs = ([], [], [("xif",)], [("xi", 1)])[rx]
        after = ["own_tokens"] if rx == 0 else ["x_ids", ("", "x_tok_0", "x_far", "x_tok_1")[rx]]

        @step(1.1, 20, f"take_{rx}", needs, after, [("rs", rx), ("rm", rx), ("rc", OWN, rx)])
        def _():
            n = normed(rx, 0)
            logits = lax.dot_general(n, router[...], NT, preferred_element_type=F32)
            columns = lax.dot_general(
                eye, idt[rx].astype(F32).astype(BF16), NT, preferred_element_type=F32
            )
            id0, id1 = columns[:, 0:1], columns[:, 1:2]
            l0 = jnp.sum(jnp.where(lane8 == id0, logits, 0.0), axis=-1, keepdims=True)
            l1 = jnp.sum(jnp.where(lane8 == id1, logits, 0.0), axis=-1, keepdims=True)
            w0 = jax.nn.sigmoid(l0 - l1)
            span = pl.ds(rx * CAP, CAP)
            for k in (1, 0):
                is0, is1 = id0 == experts[k], id1 == experts[k]
                wcol[k, rx] = jnp.where(is0, w0, 0.0) + jnp.where(is1, 1.0 - w0, 0.0)
                named = jnp.where(is0, 1.0, 0.0) + jnp.where(is1, 1.0, 0.0)
                named = jnp.broadcast_to(named, (TOK, TOK))
                slot = dot(earlier, named.astype(BF16))
                chosen = jnp.where(slot == lane, named, 0.0)
                sel[k, rx] = chosen.astype(BF16)
                table = jnp.transpose(chosen)[0:CAP, :].astype(BF16)
                found = dot(table, n).astype(BF16)
                if k == 0:
                    rows[OWN, 0, span, :] = found
                else:
                    frow[span, :] = found

    def take_other(rx):
        @step(0.35, 35, f"other_{rx}", [("ct", rx)])
        def _():
            normed(rx, 1)

    def shared_pair(rx):
        @step(1.07, 50, f"shared_{rx}", [], ["own_shared", f"take_{rx}", f"other_{rx}"], [("sc", rx)])
        def _():
            a = xn[pl.ds(rx * 2 * TOK, 2 * TOK), :]
            hidden = silu_mul(dot(a, sgw[...]), dot(a, suw[...]))
            part = dot(hidden, sdw[...])
            sown[rx] = part[:TOK] * gcol[2 * rx]
            ssend[rx] = (part[TOK:] * gcol[2 * rx + 1]).astype(BF16)

    every_row = []
    for rx in range(XN):
        take_block(rx)
        take_other(rx)
        shared_pair(rx)
        passing(4, f"rows_mate_{rx}", [("rm", rx)], [("rc", MATE, rx)])
        passing(4, f"rows_swap_{rx}", [("rs", rx)], [("rf", rx), ("rc", SWAP, rx)])
        passing(4, f"rows_opp_{rx}", [("rf", rx)], [("rc", OPP, rx)])
        every_row += [("rc", pos, rx) for pos in range(YN)]
    rows_here = [f"rows_{k}_{rx}" for k in ("mate", "swap", "opp") for rx in range(XN)]

    of_slot = {s: [] for s in range(ZN)}
    for kind in "nf":
        of_slot[0] += [f"z{kind}_own_{which}" for which in range(2)]
        for hop in range(1, 5):
            for which in range(2):
                for way in range(2):
                    if ("zw", way, hop, which) in links.copies:
                        onward = [("zw", way, hop + 1, which)]
                        onward = [n for n in onward if n in links.copies]
                        name = f"z{kind}_{way}_{hop}_{which}"
                        passing(0, name, [("zw", way, hop, which)], onward, kind=kind)
                        of_slot[z_slot(way, hop)].append(name)
    for c in range(NC):
        for way in range(2):
            for kind in "nf":
                here = "own_down_first" if kind == "f" and c == 0 else f"own_down_{kind}"
                passing(1, f"d{kind}_{way}_1_{c}", [], [("zd", way, 1, c)], [here], kind)
            for hop in range(2, 5):
                if ("zd", way, hop, c) in links.copies:
                    passing(1, f"d_{way}_{hop}_{c}", [("zd", way, hop - 1, c)], [("zd", way, hop, c)])

    def gate_up(s):
        @step(1.0, 30, f"gate_up_{s}", every_row, of_slot[s] + rows_here)
        def _():
            for k in range(YN):
                both = dot(rows[k].reshape(ROWS, D), gu[s])
                hid[pl.ds(k * ROWS, ROWS), pl.ds(s * HID, HID)] = silu_mul(both[:, :HID], both[:, HID:])

    for s in (0, 1, 7, 2, 6, 3, 5, 4):
        gate_up(s)
    hidden_done = [f"gate_up_{s}" for s in range(ZN)]

    def way_back(c):
        columns = COLUMNS[c]
        needs = [n for n in links.copies if n[0] == "zd" and n[3] == c]

        def down_out(first, many):
            h = hid[pl.ds(first * ROWS, many * ROWS), :]
            part = lax.dot_general(h, dn[columns, :], NT, preferred_element_type=F32)
            for k in range(many):
                pown[first + k, :, columns] = part[k * ROWS : k * ROWS + HALF_R]
                psend[first + k, :, columns] = part[k * ROWS + HALF_R : (k + 1) * ROWS].astype(BF16)

        @step(0.6, 24, f"far_{c}", needs, hidden_done + ["own_down_n", "own_down_f"], [("pf", c)])
        def _():
            down_out(OPP, 1)

        @step(1.4, 25, f"near_{c}", [], [f"far_{c}"], [("pn", c)])
        def _():
            down_out(MATE, 3)

    def home(c, p):
        columns = PARTS[c][p]

        def chip(pos):
            return pown[pos, :, columns] + precv[pos, :, columns].astype(F32)

        @step(0.1, 9, f"opp_{c}_{p}", [("pf", c)], [f"near_{c}"], [("y1", c, p)])
        def _():
            y1s[:, columns] = chip(OPP).astype(BF16)

        @step(0.1, 9, f"mate_{c}_{p}", [("pn", c)], [f"near_{c}"], [("y2", c, p)])
        def _():
            y2s[:, columns] = chip(MATE).astype(BF16)

        @step(0.1, 8, f"swap_{c}_{p}", [("y1", c, p), ("pn", c)], [f"near_{c}"], [("y3", c, p)])
        def _():
            y3s[:, columns] = (chip(SWAP) + y1r[:, columns].astype(F32)).astype(BF16)

        @step(
            0.45, 8, f"combine_{c}_{p}",
            [("y2", c, p), ("y3", c, p), ("pn", c)] + [("sc", rx) for rx in range(XN)],
            [f"near_{c}"] + [f"shared_{rx}" for rx in range(XN)],
            [("x1", 0, c, p), ("x1", 1, c, p), ("x2", 0, c, p), ("x2", 1, c, p)],
        )
        def _():
            rrow[:, columns] = (chip(OWN) + y2r[:, columns].astype(F32)).astype(BF16)

            def part(rx):
                span = pl.ds(rx * CAP, CAP)
                here = dot(sel[0, rx][:, :CAP], rrow[span, columns]) * wcol[0, rx]
                there = dot(sel[1, rx][:, :CAP], y3r[span, columns]) * wcol[1, rx]
                return here + there + sown[rx, :, columns] + srecv[rx, :, columns].astype(F32)

            far = part(2)
            xs1[0, :, columns] = far[:HALF_T].astype(BF16)
            xs1[1, :, columns] = far[HALF_T:].astype(BF16)
            after = part(3)
            xs2[0, :, columns] = after[HALF_T:].astype(BF16)
            xmerge[0, :, columns] = after[:HALF_T]
            before = part(1)
            xs2[1, :, columns] = before[:HALF_T].astype(BF16)
            xmerge[1, :, columns] = before[HALF_T:]
            cown[:, columns] = part(0)

        def x_merge(way):
            @step(0.06, 7, f"x_merge_{way}_{c}_{p}", [("x1", way, c, p)], [f"combine_{c}_{p}"], [("x3", way, c, p)])
            def _():
                xs3[way, :, columns] = (
                    xmerge[way, :, columns] + xr1[way, :, columns].astype(F32)
                ).astype(BF16)

        x_merge(0)
        x_merge(1)

        @step(0.1, 12, f"finish_{c}_{p}", [(k, way, c, p) for k in ("x2", "x3") for way in range(2)], [f"combine_{c}_{p}"])
        def _():
            own = cown[:, columns]
            out[pl.ds(0, HALF_T), columns] = (
                own[:HALF_T] + xr3[0, :, columns].astype(F32) + xr2[1, :, columns].astype(F32)
            ).astype(BF16)
            out[pl.ds(HALF_T, HALF_T), columns] = (
                own[HALF_T:] + xr2[0, :, columns].astype(F32) + xr3[1, :, columns].astype(F32)
            ).astype(BF16)

    for c in range(NC):
        way_back(c)
        for p in range(len(PARTS[c])):
            home(c, p)

    only = {"n": native, "f": foreign}
    for name in plan.order():
        run, _, _, needs, _, sends, kind = plan.tasks[name]

        def carry_out(run=run, needs=needs, sends=sends, name=name, kind=kind):
            for n in needs:
                links.arrive(n, kind)
            with jax.named_scope(name):
                run()
            for n in sends:
                links.send(n, kind)

        if kind is None:
            carry_out()
        else:
            pl.when(only[kind])(carry_out)
    for name in links.copies:
        whole = ({None}, {"f"} if name[0] == "w" else {"n", "f"})
        assert {k for m, k in links.started if m == name} in whole
        assert {k for m, k in links.arrived if m == name} in whole
    with jax.named_scope("finish"):

        @pl.when(foreign)
        def _():
            for k in range(len(own_weights)):
                links.copies["w", k].wait_send()

        for name, copy in links.copies.items():
            if name[0] != "w":
                copy.wait_send()


def body(
    tokens,
    norm_gain,
    router_weight,
    shared_gate_vector,
    expert_ids,
    gate_weight,
    up_weight,
    down_weight,
    shared_gate_weight,
    shared_up_weight,
    shared_down_weight,
):
    anywhere = pl.BlockSpec(memory_space=pl.ANY)
    inside = pl.BlockSpec(memory_space=pltpu.VMEM)
    vmem = pltpu.VMEM
    return pl.pallas_call(
        layer_kernel,
        out_shape=pltpu.VMEM((TOK, D), BF16),
        in_specs=[anywhere, anywhere, inside, inside, inside] + [anywhere] * 6,
        out_specs=inside,
        scratch_shapes=[
            vmem((XN, CN, TOK, D), BF16),
            vmem((XN, 2, TOK), jnp.int32),
            vmem((BLOCKS * TOK, D), BF16),
            vmem((2, XN, TOK, TOK), BF16),
            vmem((2, XN, TOK, 1), F32),
            vmem((BLOCKS, TOK, 1), F32),
            vmem((YN, 2, HALF_R, D), BF16),
            vmem((HALF_R, D), BF16),
            vmem((ZN, D, 2 * HID), BF16),
            vmem((D, ZN * HID), BF16),
            vmem((YN * ROWS, ZN * HID), BF16),
            vmem((D, SHID), BF16),
            vmem((D, SHID), BF16),
            vmem((SHID, D), BF16),
            vmem((XN, TOK, D), F32),
            vmem((XN, TOK, D), BF16),
            vmem((XN, TOK, D), BF16),
            vmem((YN, HALF_R, D), F32),
            vmem((YN, HALF_R, D), BF16),
            vmem((YN, HALF_R, D), BF16),
        ]
        + [vmem((HALF_R, D), BF16)] * 7
        + [vmem((TOK, D), F32), vmem((2, HALF_T, D), F32)]
        + [vmem((2, HALF_T, D), BF16)] * 6
        + [vmem((3, D, HID), BF16)]
        + [
            pltpu.SemaphoreType.DMA((9,)),
            pltpu.SemaphoreType.DMA((COPIES,)),
            pltpu.SemaphoreType.DMA((COPIES,)),
        ],
        compiler_params=pltpu.CompilerParams(
            collective_id=0, has_side_effects=True, vmem_limit_bytes=60 * 1024 * 1024
        ),
        name="moe_layer",
    )(
        tokens,
        expert_ids.T,
        norm_gain.reshape(1, D),
        router_weight.T,
        shared_gate_vector.reshape(1, D),
        gate_weight.reshape(D, HID),
        up_weight.reshape(D, HID),
        down_weight.reshape(D, HID),
        shared_gate_weight,
        shared_up_weight,
        shared_down_weight,
    )


def solution(mesh):
    return jax.shard_map(
        body,
        mesh=mesh,
        in_specs=(
            P(("expert", "dp"), None),
            P(),
            P(),
            P(),
            P(("expert", "dp"), None),
            P("expert", None, "dp"),
            P("expert", None, "dp"),
            P("expert", None, "dp"),
            P(None, "expert"),
            P(None, "expert"),
            P("expert", None),
        ),
        out_specs=P(("expert", "dp"), None),
        check_vma=False,
    )
```

```python
import jax
import jax.numpy as jnp
from jax import lax
from jax.experimental import pallas as pl
from jax.experimental.pallas import tpu as pltpu
from jax.sharding import PartitionSpec as P

MESH = pl.DeviceIdType.MESH
BF16 = jnp.bfloat16
F32 = jnp.float32

XN, CN, YN, ZN = 4, 2, 4, 8
TOK = 128
D = 1024
HID = 128
SHID = 512
CAP = 48
BLOCKS = XN * CN
ROWS = BLOCKS * CAP
WIDTHS = (256, 256, 256, 256)
NC = len(WIDTHS)
COLUMNS = tuple(pl.ds(sum(WIDTHS[:c]), WIDTHS[c]) for c in range(NC))
OTHERS = pl.ds(WIDTHS[0], D - WIDTHS[0])
OPP, MATE, SWAP, OWN = range(YN)
HALF_R = ROWS // 2
HALF_T = TOK // 2
COPIES = 256

NT = (((1,), (1,)), ((), ()))


def dot(a, b):
    return jnp.dot(a, b, preferred_element_type=F32)


class Links:
    def __init__(self, send_sem, recv_sem):
        self.send_sem, self.recv_sem = send_sem, recv_sem
        self.copies, self.started, self.arrived = {}, set(), set()

    def add(self, name, link, src, dst, device):
        k = len(self.copies)
        self.copies[name] = pltpu.make_async_remote_copy(
            src_ref=src,
            dst_ref=dst,
            send_sem=self.send_sem.at[k],
            recv_sem=self.recv_sem.at[k],
            device_id=device,
            device_id_type=MESH,
        )

    def send(self, name, kind=None):
        assert (name, kind) not in self.started
        self.started.add((name, kind))
        self.copies[name].start()

    def arrive(self, name, kind=None):
        if (name, kind) not in self.arrived and (name, None) not in self.arrived:
            self.arrived.add((name, kind))
            with jax.named_scope("w_" + "_".join(map(str, name))):
                self.copies[name].wait_recv()


STEPS = (
    3, 0, 2, 7, 5, 10, 76, 98, 85, 90, 4, 15, 41, 67, 12, 42, 13, 6, 11, 33, 8, 1, 39, 40, 14, 27, 54, 53, 22, 37, 21,
    56, 80, 28, 29, 45, 16, 23, 19, 9, 91, 72, 68, 30, 34, 81, 86, 25, 43, 55, 57, 38, 58, 18, 24, 31, 35, 20, 77, 44,
    46, 59, 73, 36, 17, 82, 60, 69, 87, 26, 50, 61, 74, 32, 104, 70, 99, 83, 103, 63, 64, 78, 107, 49, 47, 65, 62, 48,
    109, 105, 75, 100, 71, 94, 95, 108, 106, 88, 79, 52, 92, 66, 84, 51, 110, 112, 111, 114, 113, 96, 101, 93, 89,
    115, 121, 122, 97, 102, 123, 130, 124, 131, 132, 139, 116, 140, 141, 133, 125, 142, 134, 117, 143, 126, 135, 127,
    128, 144, 137, 136, 118, 119, 145, 146, 120, 129, 138, 147,
)


class Plan:
    def __init__(self):
        self.tasks = {}

    def task(self, name, run, us, rank, needs=(), after=(), sends=(), kind=None):
        assert name not in self.tasks
        self.tasks[name] = (run, us, rank, tuple(needs), tuple(after), tuple(sends), kind)

    def order(self):
        names = list(self.tasks)
        assert sorted(STEPS) == list(range(len(names)))
        done = set()
        for name in (names[k] for k in STEPS):
            assert done.issuperset(self.tasks[name][4])
            done.add(name)
            yield name


def silu_mul(g, u):
    return (g * jax.nn.sigmoid(g) * u).astype(BF16)


def layer_kernel(
    tokens, ids, gain, router, gate_vector, gate, up, down, sgate, sup, sdown, out,
    tok, idt, xn, sel, wcol, gcol, rows, frow, gu, dn, hid, sgw, suw, sdw,
    sown, ssend, srecv, pown, psend, precv, rrow, y1s, y2s, y3s, y1r, y2r, y3r,
    cown, xmerge, xs1, xs2, xs3, xr1, xr2, xr3, aside,
    local_sem, send_sem, recv_sem,
):
    e, d = lax.axis_index("expert"), lax.axis_index("dp")
    x, core = lax.div(e, CN), lax.rem(e, CN)
    y, z = lax.div(d, ZN), lax.rem(d, ZN)
    role, odd = lax.div(y, 2), lax.rem(y, 2)
    mate_y = y + 1 - 2 * odd
    swap_y = lax.rem(y + 3 + 2 * odd, YN)
    native, foreign = core == role, core != role

    def step_x(by):
        return (lax.rem(x + by, XN) * CN + core, d)

    def step_z(by):
        return (e, y * ZN + lax.rem(z + by, ZN))

    to_x = (step_x(1), step_x(XN - 1))
    to_z = (step_z(1), step_z(ZN - 1))
    mate, swap = (e, mate_y * ZN + z), (e, swap_y * ZN + z)
    partner = (x * CN + (1 - core), d)
    cross = (x * CN + (1 - core), swap_y * ZN + z)

    first_lanes = pl.ds(0, HID)
    own_weights = (
        (gate, gu.at[0, :, first_lanes]),
        (up, gu.at[0, :, pl.ds(HID, HID)]),
        (down.at[COLUMNS[0]], dn.at[COLUMNS[0], first_lanes]),
        (down.at[OTHERS], dn.at[OTHERS, first_lanes]),
    )
    pairs = ((tokens, tok.at[0, 0]), (ids, idt.at[0]), *own_weights, (sgate, sgw), (sup, suw), (sdown, sdw))
    local = [pltpu.make_async_copy(src, dst, local_sem.at[i]) for i, (src, dst) in enumerate(pairs)]
    for i in (0, 1):
        local[i].start()

    given = ((gate, aside.at[0]), (up, aside.at[1]), (down, aside.at[2]))
    lent = [pltpu.make_async_copy(src, dst, local_sem.at[2 + i]) for i, (src, dst) in enumerate(given)]

    @pl.when(native)
    def _():
        for i in (2, 3, 4, 5):
            local[i].start()

    @pl.when(foreign)
    def _():
        for copy in lent:
            copy.start()

    for i in (6, 7, 8):
        local[i].start()

    barrier = pltpu.get_barrier_semaphore()
    for device in (*to_x, *to_z, partner, mate, swap, cross):
        pl.semaphore_signal(barrier, inc=1, device_id=device, device_id_type=MESH)
    with jax.named_scope("meet"):
        pl.semaphore_wait(barrier, 8)

    links = Links(send_sem, recv_sem)
    add = links.add

    near = (1, 3)
    lo, hi = pl.ds(0, HALF_T), pl.ds(HALF_T, HALF_T)
    for way in range(2):
        add(("xt", way), f"x{way}", tok.at[0, 0], tok.at[near[way], 0], to_x[way])
        add(("xi", way), f"x{way}", idt.at[0], idt.at[near[way]], to_x[way])
        part = (lo, hi)[way]
        add(("xf", way), f"x{way}", tok.at[near[way], 0, part], tok.at[2, 0, part], to_x[way])
    add(("xif",), "x0", idt.at[1], idt.at[2], to_x[0])
    for rx in range(XN):
        add(("ct", rx), "c", tok.at[rx, 0], tok.at[rx, 1], partner)

    for rx in range(XN):
        span = pl.ds(rx * CAP, CAP)
        add(("rs", rx), "s", frow.at[span], rows.at[SWAP, 0, span], swap)
        add(("rm", rx), "y", rows.at[OWN, 0, span], rows.at[MATE, 0, span], mate)
        add(("rf", rx), "y", rows.at[SWAP, 0, span], rows.at[OPP, 0, span], mate)
        for pos in range(YN):
            add(("rc", pos, rx), "c", rows.at[pos, 0, span], rows.at[pos, 1, span], partner)

    sources = (aside.at[0], aside.at[1], aside.at[2, COLUMNS[0]], aside.at[2, OTHERS])
    for k, (src, (_, dst)) in enumerate(zip(sources, own_weights)):
        add(("w", k), "s", src, dst, cross)

    def z_slot(way, hop):
        return hop if way == 0 else (ZN - hop) % ZN

    lanes = (first_lanes, pl.ds(HID, HID))
    for hop in range(1, 5):
        for way in range(2):
            src, dst = z_slot(way, hop - 1), z_slot(way, hop)
            for which in range(2):
                if hop < 4 or which == way:
                    add(("zw", way, hop, which), f"z{way}", gu.at[src, :, lanes[which]], gu.at[dst, :, lanes[which]], to_z[way])
            for c in range(NC):
                if hop < 4 or c % 2 == way:
                    span = COLUMNS[c]
                    add(
                        ("zd", way, hop, c),
                        f"z{way}",
                        dn.at[span, pl.ds(src * HID, HID)],
                        dn.at[span, pl.ds(dst * HID, HID)],
                        to_z[way],
                    )

    for rx in range(XN):
        add(("sc", rx), "c", ssend.at[rx], srecv.at[rx], partner)
    for c in range(NC):
        cols = COLUMNS[c]
        add(("pf", c), "c", psend.at[OPP, :, cols], precv.at[OPP, :, cols], partner)
        rest = pl.ds(MATE, 3)
        add(("pn", c), "c", psend.at[rest, :, cols], precv.at[rest, :, cols], partner)
        add(("y1", c), "y", y1s.at[:, cols], y1r.at[:, cols], mate)
        add(("y2", c), "y", y2s.at[:, cols], y2r.at[:, cols], mate)
        add(("y3", c), "s", y3s.at[:, cols], y3r.at[:, cols], swap)
        for way in range(2):
            add(("x1", way, c), f"x{way}", xs1.at[way, :, cols], xr1.at[way, :, cols], to_x[way])
            add(("x2", way, c), f"x{way}", xs2.at[way, :, cols], xr2.at[way, :, cols], to_x[way])
            add(("x3", way, c), f"x{way}", xs3.at[way, :, cols], xr3.at[way, :, cols], to_x[way])
    assert len(links.copies) <= COPIES

    row_iota = lax.broadcasted_iota(jnp.int32, (TOK, TOK), 0)
    lane_iota = lax.broadcasted_iota(jnp.int32, (TOK, TOK), 1)
    eye = jnp.where(row_iota == lane_iota, 1.0, 0.0).astype(BF16)
    earlier = jnp.where(lane_iota < row_iota, 1.0, 0.0).astype(BF16)
    lane = lane_iota.astype(F32)
    lane8 = lax.broadcasted_iota(jnp.int32, (TOK, BLOCKS), 1).astype(F32)
    experts = ((x * CN + role).astype(F32), (x * CN + 1 - role).astype(F32))
    plan = Plan()

    def step(us, rank, name, needs=(), after=(), sends=(), kind=None):
        def keep(run):
            plan.task(name, run, us, rank, needs, after, sends, kind)

        return keep

    def passing(rank, name, needs, sends, after=(), kind=None):
        plan.task(name, lambda: None, 0.03, rank, needs, after, sends, kind)

    @step(0.03, 0, "swap_weights", sends=[("w", 0), ("w", 1), ("w", 2)], kind="f")
    def _():
        for copy in lent:
            copy.wait()

    passing(0, "swap_down", [], [("w", 3)], ["take_3"], "f")

    @step(0.05, 0, "own_tokens", sends=[("xi", 0), ("xt", 0), ("xi", 1), ("xt", 1), ("ct", 0)])
    def _():
        local[0].wait()
        local[1].wait()

    for which in range(2):
        both_ways = [("zw", way, 1, which) for way in range(2)]

        @step(0.05, 1, f"zn_own_{which}", sends=both_ways, kind="n")
        def _(which=which):
            local[2 + which].wait()

        passing(0, f"zf_own_{which}", [("w", which)], both_ways, kind="f")

    @step(0.05, 3, "own_down_n", kind="n")
    def _():
        local[4].wait()
        local[5].wait()

    passing(1, "own_down_first", [("w", 2)], [], kind="f")
    passing(3, "own_down_f", [("w", 3)], [], ["own_down_first"], "f")

    @step(0.05, 40, "own_shared")
    def _():
        for i in (6, 7, 8):
            local[i].wait()

    passing(1, "x_ids", [("xi", 0)], [("xif",)])
    for way in range(2):
        passing(2, f"x_tok_{way}", [("xt", way)], [("xf", way), ("ct", near[way])])
    passing(2, "x_far", [("xf", 0), ("xf", 1)], [("ct", 2)])

    def normed(rx, cc):
        wide = tok[rx, cc].astype(F32)
        mean_square = jnp.mean(wide * wide, axis=-1, keepdims=True)
        n = (wide * lax.rsqrt(mean_square + 1e-06) * gain[...]).astype(BF16)
        b = 2 * rx + cc
        xn[pl.ds(b * TOK, TOK), :] = n
        gcol[b] = jax.nn.sigmoid(
            jnp.sum(n.astype(F32) * gate_vector[...], axis=-1, keepdims=True)
        )
        return n

    def take_block(rx):
        needs = ([], [], [("xif",)], [("xi", 1)])[rx]
        after = ["own_tokens"] if rx == 0 else ["x_ids", ("", "x_tok_0", "x_far", "x_tok_1")[rx]]

        @step(1.1, 20, f"take_{rx}", needs, after, [("rs", rx), ("rm", rx), ("rc", OWN, rx)])
        def _():
            n = normed(rx, 0)
            logits = lax.dot_general(n, router[...], NT, preferred_element_type=F32)
            columns = lax.dot_general(
                eye, idt[rx].astype(F32).astype(BF16), NT, preferred_element_type=F32
            )
            id0, id1 = columns[:, 0:1], columns[:, 1:2]
            l0 = jnp.sum(jnp.where(lane8 == id0, logits, 0.0), axis=-1, keepdims=True)
            l1 = jnp.sum(jnp.where(lane8 == id1, logits, 0.0), axis=-1, keepdims=True)
            w0 = jax.nn.sigmoid(l0 - l1)
            span = pl.ds(rx * CAP, CAP)
            for k in (1, 0):
                is0, is1 = id0 == experts[k], id1 == experts[k]
                wcol[k, rx] = jnp.where(is0, w0, 0.0) + jnp.where(is1, 1.0 - w0, 0.0)
                named = jnp.where(is0, 1.0, 0.0) + jnp.where(is1, 1.0, 0.0)
                named = jnp.broadcast_to(named, (TOK, TOK))
                slot = dot(earlier, named.astype(BF16))
                chosen = jnp.where(slot == lane, named, 0.0)
                sel[k, rx] = chosen.astype(BF16)
                table = jnp.transpose(chosen)[0:CAP, :].astype(BF16)
                found = dot(table, n).astype(BF16)
                if k == 0:
                    rows[OWN, 0, span, :] = found
                else:
                    frow[span, :] = found

    def take_other(rx):
        @step(0.35, 35, f"other_{rx}", [("ct", rx)])
        def _():
            normed(rx, 1)

    def shared_pair(rx):
        @step(1.07, 50, f"shared_{rx}", [], ["own_shared", f"take_{rx}", f"other_{rx}"], [("sc", rx)])
        def _():
            a = xn[pl.ds(rx * 2 * TOK, 2 * TOK), :]
            hidden = silu_mul(dot(a, sgw[...]), dot(a, suw[...]))
            part = dot(hidden, sdw[...])
            sown[rx] = part[:TOK] * gcol[2 * rx]
            ssend[rx] = (part[TOK:] * gcol[2 * rx + 1]).astype(BF16)

    every_row = []
    for rx in range(XN):
        take_block(rx)
        take_other(rx)
        shared_pair(rx)
        passing(4, f"rows_mate_{rx}", [("rm", rx)], [("rc", MATE, rx)])
        passing(4, f"rows_swap_{rx}", [("rs", rx)], [("rf", rx), ("rc", SWAP, rx)])
        passing(4, f"rows_opp_{rx}", [("rf", rx)], [("rc", OPP, rx)])
        every_row += [("rc", pos, rx) for pos in range(YN)]
    rows_here = [f"rows_{k}_{rx}" for k in ("mate", "swap", "opp") for rx in range(XN)]

    of_slot = {s: [] for s in range(ZN)}
    for kind in "nf":
        of_slot[0] += [f"z{kind}_own_{which}" for which in range(2)]
        for hop in range(1, 5):
            for which in range(2):
                for way in range(2):
                    if ("zw", way, hop, which) in links.copies:
                        onward = [("zw", way, hop + 1, which)]
                        onward = [n for n in onward if n in links.copies]
                        name = f"z{kind}_{way}_{hop}_{which}"
                        passing(0, name, [("zw", way, hop, which)], onward, kind=kind)
                        of_slot[z_slot(way, hop)].append(name)
    for c in range(NC):
        for way in range(2):
            for kind in "nf":
                here = "own_down_first" if kind == "f" and c == 0 else f"own_down_{kind}"
                passing(1, f"d{kind}_{way}_1_{c}", [], [("zd", way, 1, c)], [here], kind)
            for hop in range(2, 5):
                if ("zd", way, hop, c) in links.copies:
                    passing(1, f"d_{way}_{hop}_{c}", [("zd", way, hop - 1, c)], [("zd", way, hop, c)])

    def gate_up(s):
        @step(1.0, 30, f"gate_up_{s}", every_row, of_slot[s] + rows_here)
        def _():
            products(s, (OPP,) if s == 4 else range(YN))

    def products(s, positions):
        for k in positions:
            both = dot(rows[k].reshape(ROWS, D), gu[s])
            hid[pl.ds(k * ROWS, ROWS), pl.ds(s * HID, HID)] = silu_mul(both[:, :HID], both[:, HID:])

    for s in (0, 1, 7, 2, 6, 3, 5, 4):
        gate_up(s)
    @step(0.8, 23, "gate_up_rest", [], ["gate_up_4", "far_0"])
    def _():
        products(4, (MATE, SWAP, OWN))

    hidden_done = [f"gate_up_{s}" for s in range(ZN)]

    def way_back(c):
        columns = COLUMNS[c]
        needs = [n for n in links.copies if n[0] == "zd" and n[3] == c]

        def down_out(first, many):
            h = hid[pl.ds(first * ROWS, many * ROWS), :]
            part = lax.dot_general(h, dn[columns, :], NT, preferred_element_type=F32)
            for k in range(many):
                pown[first + k, :, columns] = part[k * ROWS : k * ROWS + HALF_R]
                psend[first + k, :, columns] = part[k * ROWS + HALF_R : (k + 1) * ROWS].astype(BF16)

        def chip(pos):
            return pown[pos, :, columns] + precv[pos, :, columns].astype(F32)

        @step(0.6, 24, f"far_{c}", needs, hidden_done + ["own_down_n", "own_down_f"], [("pf", c)])
        def _():
            down_out(OPP, 1)

        @step(1.4, 25, f"near_{c}", [], [f"far_{c}", "gate_up_rest"], [("pn", c)])
        def _():
            down_out(MATE, 3)

        @step(0.1, 9, f"opp_{c}", [("pf", c)], [f"far_{c}"], [("y1", c)])
        def _():
            y1s[:, columns] = chip(OPP).astype(BF16)

        @step(0.1, 9, f"mate_{c}", [("pn", c)], [f"near_{c}"], [("y2", c)])
        def _():
            y2s[:, columns] = chip(MATE).astype(BF16)

        @step(0.1, 8, f"swap_{c}", [("y1", c), ("pn", c)], [f"near_{c}"], [("y3", c)])
        def _():
            y3s[:, columns] = (chip(SWAP) + y1r[:, columns].astype(F32)).astype(BF16)

        @step(
            0.45, 8, f"combine_{c}",
            [("y2", c), ("y3", c), ("pn", c)] + [("sc", rx) for rx in range(XN)],
            [f"near_{c}"] + [f"shared_{rx}" for rx in range(XN)],
            [("x1", 0, c), ("x1", 1, c), ("x2", 0, c), ("x2", 1, c)],
        )
        def _():
            rrow[:, columns] = (chip(OWN) + y2r[:, columns].astype(F32)).astype(BF16)

            def part(rx):
                span = pl.ds(rx * CAP, CAP)
                here = dot(sel[0, rx][:, :CAP], rrow[span, columns]) * wcol[0, rx]
                there = dot(sel[1, rx][:, :CAP], y3r[span, columns]) * wcol[1, rx]
                return here + there + sown[rx, :, columns] + srecv[rx, :, columns].astype(F32)

            far = part(2)
            xs1[0, :, columns] = far[:HALF_T].astype(BF16)
            xs1[1, :, columns] = far[HALF_T:].astype(BF16)
            after = part(3)
            xs2[0, :, columns] = after[HALF_T:].astype(BF16)
            xmerge[0, :, columns] = after[:HALF_T]
            before = part(1)
            xs2[1, :, columns] = before[:HALF_T].astype(BF16)
            xmerge[1, :, columns] = before[HALF_T:]
            cown[:, columns] = part(0)

        def x_merge(way):
            @step(0.06, 7, f"x_merge_{way}_{c}", [("x1", way, c)], [f"combine_{c}"], [("x3", way, c)])
            def _():
                xs3[way, :, columns] = (
                    xmerge[way, :, columns] + xr1[way, :, columns].astype(F32)
                ).astype(BF16)

        x_merge(0)
        x_merge(1)

        @step(0.1, 12, f"finish_{c}", [(k, way, c) for k in ("x2", "x3") for way in range(2)], [f"combine_{c}"])
        def _():
            own = cown[:, columns]
            out[pl.ds(0, HALF_T), columns] = (
                own[:HALF_T] + xr3[0, :, columns].astype(F32) + xr2[1, :, columns].astype(F32)
            ).astype(BF16)
            out[pl.ds(HALF_T, HALF_T), columns] = (
                own[HALF_T:] + xr2[0, :, columns].astype(F32) + xr3[1, :, columns].astype(F32)
            ).astype(BF16)

    for c in range(NC):
        way_back(c)

    only = {"n": native, "f": foreign}
    for name in plan.order():
        run, _, _, needs, _, sends, kind = plan.tasks[name]

        def carry_out(run=run, needs=needs, sends=sends, name=name, kind=kind):
            for n in needs:
                links.arrive(n, kind)
            with jax.named_scope(name):
                run()
            for n in sends:
                links.send(n, kind)

        if kind is None:
            carry_out()
        else:
            pl.when(only[kind])(carry_out)
    for name in links.copies:
        whole = ({None}, {"f"} if name[0] == "w" else {"n", "f"})
        assert {k for m, k in links.started if m == name} in whole
        assert {k for m, k in links.arrived if m == name} in whole
    with jax.named_scope("finish"):

        @pl.when(foreign)
        def _():
            for k in range(len(own_weights)):
                links.copies["w", k].wait_send()

        for name, copy in links.copies.items():
            if name[0] != "w":
                copy.wait_send()


def body(
    tokens,
    norm_gain,
    router_weight,
    shared_gate_vector,
    expert_ids,
    gate_weight,
    up_weight,
    down_weight,
    shared_gate_weight,
    shared_up_weight,
    shared_down_weight,
):
    anywhere = pl.BlockSpec(memory_space=pl.ANY)
    inside = pl.BlockSpec(memory_space=pltpu.VMEM)
    vmem = pltpu.VMEM
    return pl.pallas_call(
        layer_kernel,
        out_shape=pltpu.VMEM((TOK, D), BF16),
        in_specs=[anywhere, anywhere, inside, inside, inside] + [anywhere] * 6,
        out_specs=inside,
        scratch_shapes=[
            vmem((XN, CN, TOK, D), BF16),
            vmem((XN, 2, TOK), jnp.int32),
            vmem((BLOCKS * TOK, D), BF16),
            vmem((2, XN, TOK, TOK), BF16),
            vmem((2, XN, TOK, 1), F32),
            vmem((BLOCKS, TOK, 1), F32),
            vmem((YN, 2, HALF_R, D), BF16),
            vmem((HALF_R, D), BF16),
            vmem((ZN, D, 2 * HID), BF16),
            vmem((D, ZN * HID), BF16),
            vmem((YN * ROWS, ZN * HID), BF16),
            vmem((D, SHID), BF16),
            vmem((D, SHID), BF16),
            vmem((SHID, D), BF16),
            vmem((XN, TOK, D), F32),
            vmem((XN, TOK, D), BF16),
            vmem((XN, TOK, D), BF16),
            vmem((YN, HALF_R, D), F32),
            vmem((YN, HALF_R, D), BF16),
            vmem((YN, HALF_R, D), BF16),
        ]
        + [vmem((HALF_R, D), BF16)] * 7
        + [vmem((TOK, D), F32), vmem((2, HALF_T, D), F32)]
        + [vmem((2, HALF_T, D), BF16)] * 6
        + [vmem((3, D, HID), BF16)]
        + [
            pltpu.SemaphoreType.DMA((9,)),
            pltpu.SemaphoreType.DMA((COPIES,)),
            pltpu.SemaphoreType.DMA((COPIES,)),
        ],
        compiler_params=pltpu.CompilerParams(
            collective_id=0, has_side_effects=True, vmem_limit_bytes=60 * 1024 * 1024
        ),
        name="moe_layer",
    )(
        tokens,
        expert_ids.T,
        norm_gain.reshape(1, D),
        router_weight.T,
        shared_gate_vector.reshape(1, D),
        gate_weight.reshape(D, HID),
        up_weight.reshape(D, HID),
        down_weight.reshape(D, HID),
        shared_gate_weight,
        shared_up_weight,
        shared_down_weight,
    )


def solution(mesh):
    return jax.shard_map(
        body,
        mesh=mesh,
        in_specs=(
            P(("expert", "dp"), None),
            P(),
            P(),
            P(),
            P(("expert", "dp"), None),
            P("expert", None, "dp"),
            P("expert", None, "dp"),
            P("expert", None, "dp"),
            P(None, "expert"),
            P(None, "expert"),
            P("expert", None),
        ),
        out_specs=P(("expert", "dp"), None),
        check_vma=False,
    )
```
